32 devices in a mesh: section: 8 (over z, y), tensor: 4 (over x, core).
Axes of the slice: x: 2, y: 2, z: 4, core: 2. Of those that a mesh axis runs over, the one named last changes fastest.
Arguments:
- section_input: bfloat16 [8, 512, 4096], P('section', 'tensor'), may hold values from -6 to 6
- history: bfloat16 [8, 1, 512, 4096], P('section', None, 'tensor'), may hold values from -6 to 6
- query_weight: bfloat16 [8, 4096, 3072], P('section', None, 'tensor'), may hold values from -0.4 to 0.4
- key_weight: bfloat16 [8, 4096, 512], P('section', None, 'tensor'), may hold values from -0.4 to 0.4
- value_weight: bfloat16 [8, 4096, 512], P('section', None, 'tensor'), may hold values from -0.09375 to 0.09375
- output_weight: bfloat16 [8, 3072, 4096], P('section', 'tensor'), may hold values from -0.5 to 0.5
- mix_weights: float32 [8, 2], replicated, may hold values from 0.2 to 0.6
Outputs:
- next_input: bfloat16 [8, 512, 4096], P('section', 'tensor')
The draws below stay inside these ranges and needn't reach their ends.
All inputs are finite; a program needn't handle non-finite values.
Results may differ from the reference program's by a relative error of at most 0.013.
The reference program's roundings to bfloat16 on the way count: a program that leaves them out, or rounds other values in their place, can miss the bound.
Values may be sent and summed in bfloat16 or wider, within the bound.
A program may use at most 128 MiB of HBM per device.

```python
import math
import jax
import jax.numpy as jnp
from jax import lax

D = 4096
HEADS = 48
KV_HEADS = 8
HEAD_DIM = 64
DILATION_STRIDE = 4
SEQ = 512
HIST = 1
N_SECTION = 8
N_TENSOR = 4


def draw_query_weight(key, part):
    entries = jax.random.normal(jax.random.fold_in(key, 11), (N_SECTION, D, HEADS * HEAD_DIM), jnp.float32) / jnp.sqrt(jnp.float32(D))
    return jnp.clip(entries, -0.39, 0.39).astype(jnp.bfloat16)


def draw_key_weight(key, part):
    entries = jax.random.normal(jax.random.fold_in(key, 13), (N_SECTION, D, KV_HEADS * HEAD_DIM), jnp.float32) / jnp.sqrt(jnp.float32(D))
    return jnp.clip(entries, -0.39, 0.39).astype(jnp.bfloat16)


def steps_of(rng, extent, shards, low, high):
    level, own = 1.0, jax.random.fold_in(rng, 6)
    for dim, shards_of in shards:
        heights = jnp.exp(jax.random.uniform(jax.random.fold_in(own, dim), (shards_of,), jnp.float32, low / len(shards), high / len(shards)))
        level = level * jnp.repeat(heights, extent[dim] // shards_of).reshape([-1 if axis == dim else 1 for axis in range(len(extent))])
    return level


def noise(key, shape, spread, reach, shards=(), kind=jnp.bfloat16):
    factor_of = steps_of(key, shape, shards, -0.22, 0.18) if shards else 1.0
    result = jax.random.normal(key, shape, jnp.float32) * spread * factor_of
    return jnp.minimum(jnp.maximum(result, -reach), reach).astype(kind)


def setup_inputs(seed: int = 0) -> dict:
    seeds = jax.random.split(jax.random.key(seed), 8)
    return {
        "section_input": noise(seeds[0], (N_SECTION, SEQ, D), 1.0, 6.0, ((0, 8), (1, 4))),
        "history": noise(seeds[1], (N_SECTION, HIST, SEQ, D), 1.0, 6.0, ((0, 8), (2, 4))),
        "query_weight": draw_query_weight(jax.random.fold_in(seeds[7], 71), 0),
        "key_weight": draw_key_weight(jax.random.fold_in(seeds[7], 71), 0),
        "value_weight": noise(seeds[4], (N_SECTION, D, KV_HEADS * HEAD_DIM), D ** -0.5, 0.09375, ((0, 8), (2, 4))),
        "output_weight": noise(seeds[5], (N_SECTION, HEADS * HEAD_DIM, D), 0.08, 0.5, ((0, 8), (1, 4))),
        "mix_weights": jnp.clip(jax.random.uniform(seeds[6], (N_SECTION, HIST + 1), jnp.float32, 0.2, 0.6), 0.2, 0.6),
    }


def normalize(token_rows):
    values = token_rows.astype(jnp.float32)
    inv_scale = lax.rsqrt(lax.optimization_barrier(jnp.mean(values * values, axis=-1, keepdims=True)) + 1e-05)
    return (values * inv_scale).astype(jnp.bfloat16)

def one_section(operands):
    token_rows, query_part, key_part, value_part, output_part = operands
    seq_len = token_rows.shape[0]
    normed = normalize(token_rows)
    query_rows = jnp.dot(normed, query_part, preferred_element_type=jnp.float32).astype(jnp.bfloat16)
    key_rows = jnp.dot(normed, key_part, preferred_element_type=jnp.float32).astype(jnp.bfloat16)
    value_rows = jnp.dot(normed, value_part, preferred_element_type=jnp.float32).astype(jnp.bfloat16)
    per_group = HEADS // KV_HEADS
    query_heads = query_rows.astype(jnp.float32).reshape(seq_len, KV_HEADS, per_group, HEAD_DIM)
    key_heads = key_rows.astype(jnp.float32).reshape(seq_len, KV_HEADS, HEAD_DIM)
    value_heads = value_rows.astype(jnp.float32).reshape(seq_len, KV_HEADS, HEAD_DIM)
    scores = jnp.einsum('tgjd,sgd->gjts', query_heads, key_heads) / math.sqrt(HEAD_DIM)
    positions = jnp.arange(seq_len, dtype=jnp.int32)
    scores = jnp.where(positions[:, None] >= positions[None, :], scores, -1e+30)
    softmax_weights = jax.nn.softmax(scores, axis=-1).astype(jnp.bfloat16)
    heads_out = jnp.einsum('gjts,sgd->tgjd', softmax_weights.astype(jnp.float32), value_heads)
    heads_out = heads_out.astype(jnp.bfloat16).reshape(seq_len, HEADS * HEAD_DIM)
    grouped = heads_out.astype(jnp.float32).reshape(seq_len, N_TENSOR, -1)
    grouped_weight = output_part.astype(jnp.float32).reshape(N_TENSOR, -1, D)
    partials = jnp.einsum('tnc,ncd->ntd', grouped, grouped_weight)
    partials = lax.optimization_barrier(partials.astype(jnp.bfloat16)).astype(jnp.float32)
    attention_sum = lax.optimization_barrier(jnp.sum(partials, axis=0))
    return (token_rows.astype(jnp.float32) + attention_sum).astype(jnp.bfloat16)

def reference(section_input, history, query_weight, key_weight, value_weight, output_weight, mix_weights):
    block_outs = lax.map(one_section, (section_input, query_weight, key_weight, value_weight, output_weight))
    section_numbers = jnp.arange(N_SECTION, dtype=jnp.int32)
    mixed_sum = mix_weights[:, 0][:, None, None] * block_outs.astype(jnp.float32)
    for history_slot in range(1, HIST + 1):
        sender_section = section_numbers - DILATION_STRIDE * history_slot
        picked = jnp.take(history[:, history_slot - 1], jnp.maximum(sender_section, 0).astype(jnp.int32), axis=0)
        factor = jnp.where(sender_section >= 0, mix_weights[:, history_slot], jnp.float32(0.0))
        mixed_sum = mixed_sum + factor[:, None, None] * picked.astype(jnp.float32)
    mixed = mixed_sum.astype(jnp.bfloat16)
    return jnp.concatenate([mixed[-1:], mixed[:-1]], axis=0)
```

```python
import functools
import math

import jax
import jax.numpy as jnp
from jax import lax
from jax.experimental import pallas as pl
from jax.experimental.pallas import tpu as pltpu
from jax.sharding import PartitionSpec as P

HEAD_DIM = 64
DILATION_STRIDE = 4
MESH = pl.DeviceIdType.MESH
UNITS = 4
DOTS = 4
CHUNKS = 8


def start(copy):
    copy.start()
    return copy


def tick_kernel(
    sections,
    x_hbm,
    hist_hbm,
    wq_hbm,
    wk_hbm,
    wv_hbm,
    wo_hbm,
    mix_hbm,
    out,
    x_own,
    x_res,
    chip_rows,
    peer_rows,
    w_all,
    w_out,
    q_all,
    k_pad,
    v_pad,
    heads,
    own_part,
    give,
    x_in,
    mixed,
    acc,
    hist_in,
    mix_v,
    w_sem,
    wo_sem,
    x_sem,
    res_sem,
    mix_sem,
    hist_s,
    hist_r,
    sib_s,
    sib_r,
    gx_s,
    gx_r,
    fw_s,
    fw_r,
    wr_s,
    wr_r,
    xr_s,
    xr_r,
    hd_s,
    hd_r,
    xs_s,
    xs_r,
    out_s,
    out_r,
):
    section = lax.axis_index("section")
    me = lax.axis_index("tensor")
    hi, lo = me // 2, me % 2
    sibling = hi * 2 + (1 - lo)
    peer = (1 - hi) * 2 + lo
    rows, width = x_own.shape
    slots = hist_in.shape[0]
    unit = rows // UNITS
    side = width // 2
    wide = side // DOTS
    cols = side // CHUNKS
    per_dot = CHUNKS // DOTS
    q_tiles = w_all.shape[0] - 1
    tile = w_all.shape[2]
    half = tile // 2
    last = sections - 1
    nxt = lax.rem(section + 1, sections)
    prv = lax.rem(section + sections - 1, sections)
    f32, bf16 = jnp.float32, jnp.bfloat16

    middle = (section > 0) & (section < last)
    gets = [middle & (section >= DILATION_STRIDE * k) for k in range(1, slots + 1)]
    gets_last = [(section == 0) & (last >= DILATION_STRIDE * k) for k in range(1, slots + 1)]
    gives = [section + DILATION_STRIDE * k < last for k in range(1, slots + 1)]
    gives_last = [section + DILATION_STRIDE * k == last for k in range(1, slots + 1)]

    load_x = start(pltpu.make_async_copy(x_hbm.at[0], x_own, x_sem))
    barrier = pltpu.get_barrier_semaphore()

    def greet(s, t):
        pl.semaphore_signal(
            barrier, inc=1, device_id={"section": s, "tensor": t}, device_id_type=MESH
        )

    greet(section, sibling)
    greet(section, peer)
    for c in range(2):
        greet(nxt, hi * 2 + c)
        greet(prv, hi * 2 + c)
    expected = jnp.int32(6)
    for k in range(1, slots + 1):
        step = DILATION_STRIDE * k

        @pl.when(gives[k - 1])
        def _():
            for c in range(2):
                greet(section + step, hi * 2 + c)

        @pl.when(gets[k - 1])
        def _():
            for c in range(2):
                greet(section - step, hi * 2 + c)

        @pl.when(gives_last[k - 1])
        def _():
            greet(0, me)

        @pl.when(gets_last[k - 1])
        def _():
            greet(last - step, me)

        expected = expected + 2 * (gives[k - 1].astype(jnp.int32) + gets[k - 1].astype(jnp.int32))
        expected = expected + gives_last[k - 1].astype(jnp.int32)
        expected = expected + gets_last[k - 1].astype(jnp.int32)

    loads = [
        pltpu.make_async_copy(
            wk_hbm.at[0], w_all.at[q_tiles, :, pl.ds(0, half)], w_sem.at[q_tiles]
        ),
        pltpu.make_async_copy(
            wv_hbm.at[0], w_all.at[q_tiles, :, pl.ds(half, half)], w_sem.at[q_tiles + 1]
        ),
    ]
    for j in range(q_tiles):
        loads.append(
            pltpu.make_async_copy(
                wq_hbm.at[0, :, pl.ds(j * tile, tile)], w_all.at[j], w_sem.at[j]
            )
        )
    load_x.wait()
    for copy in loads:
        copy.start()
    load_mix = start(pltpu.make_async_copy(mix_hbm, mix_v, mix_sem))
    mine = pl.multiple_of(lo * rows, rows)
    my_side = pl.multiple_of(lo * side, side)
    other_side = pl.multiple_of((1 - lo) * side, side)

    def norm_unit(u):
        def norm_rows(i, carry):
            at = pl.multiple_of(u * unit + i * 16, 16)
            values = x_own[pl.ds(at, 16), :].astype(f32)
            inv = lax.rsqrt(jnp.mean(values * values, axis=-1, keepdims=True) + 1e-05)
            chip_rows[pl.ds(pl.multiple_of(mine + at, 16), 16), :] = (values * inv).astype(bf16)
            return carry

        lax.fori_loop(0, unit // 16, norm_rows, 0)

    def remote(src, dst, send, recv, s, t):
        return pltpu.make_async_remote_copy(
            src_ref=src,
            dst_ref=dst,
            send_sem=send,
            recv_sem=recv,
            device_id={"section": s, "tensor": t},
            device_id_type=MESH,
        )

    def sibling_copy(u):
        place = chip_rows.at[pl.ds(pl.multiple_of(mine + u * unit, unit), unit)]
        return remote(place, place, sib_s.at[u], sib_r.at[u], section, sibling)

    def gather_copy(j, i):
        at = (2 * i + lo) * unit
        return remote(
            chip_rows.at[pl.ds(pl.multiple_of(j * rows + at, unit), unit)],
            peer_rows.at[j, pl.ds(pl.multiple_of(at, unit), unit)],
            gx_s.at[j, i],
            gx_r.at[j, i],
            section,
            peer,
        )

    def forward_copy(j, i):
        place = peer_rows.at[j, pl.ds(pl.multiple_of((2 * i + lo) * unit, unit), unit)]
        return remote(place, place, fw_s.at[j, i], fw_r.at[j, i], section, sibling)

    norm_unit(0)
    pl.semaphore_wait(barrier, expected)
    for u in range(UNITS):
        if u > 0:
            norm_unit(u)
        sibling_copy(u).start()
        if u % 2 == 0:

            @pl.when(lo == 0)
            def _():
                gather_copy(0, u // 2).start()

    @pl.when(lo == 0)
    def _():
        for i in range(UNITS // 2):
            sibling_copy(2 * i).wait_recv()
            gather_copy(1, i).start()
        for i in range(UNITS // 2):
            sibling_copy(2 * i + 1).wait_recv()

    @pl.when(lo == 1)
    def _():
        for i in range(UNITS // 2):
            sibling_copy(2 * i + 1).wait_recv()
            gather_copy(0, i).start()
        for i in range(UNITS // 2):
            gather_copy(1, i).start()
        for i in range(UNITS // 2):
            sibling_copy(2 * i).wait_recv()

    def hist_copy(k, c, q, to_last):
        src = hist_hbm.at[0, k - 1, :, pl.ds(pl.multiple_of(c * side + q * cols, cols), cols)]
        slot = c if to_last else lo
        if to_last:
            s, t = 0, me
        else:
            s, t = section + DILATION_STRIDE * k, hi * 2 + c
        return remote(
            src,
            hist_in.at[k - 1, slot, q],
            hist_s.at[k - 1, c, q],
            hist_r.at[k - 1, slot, q],
            s,
            t,
        )

    def send_history():
        for k in range(1, slots + 1):
            for to_last, sends in ((False, gives[k - 1]), (True, gives_last[k - 1])):

                @pl.when(sends)
                def _():
                    def each(q, carry):
                        for c in range(2):
                            hist_copy(k, c, q, to_last).start()
                        return carry

                    lax.fori_loop(0, CHUNKS, each, 0)

    late = (lo == 1) & (section % 2 == 0)

    @pl.when(jnp.logical_not(late))
    def _():
        send_history()

    def weight_copy(c):
        return remote(
            wo_hbm.at[0, :, pl.ds(pl.multiple_of(other_side + c * wide, wide), wide)],
            w_out.at[lo, c],
            wr_s.at[c],
            wr_r.at[c],
            section,
            sibling,
        )

    def residual_copy():
        return remote(
            x_own.at[:, pl.ds(other_side, side)], x_res.at[lo], xr_s, xr_r, section, sibling
        )

    out_loads = []
    for c in range(DOTS):
        out_loads.append(
            start(
                pltpu.make_async_copy(
                    wo_hbm.at[0, :, pl.ds(pl.multiple_of(my_side + c * wide, wide), wide)],
                    w_out.at[lo, c],
                    wo_sem.at[c],
                )
            )
        )
        weight_copy(c).start()
    load_res = start(
        pltpu.make_async_copy(x_hbm.at[0, :, pl.ds(my_side, side)], x_res.at[lo], res_sem)
    )
    residual_copy().start()

    scale = 1.0 / math.sqrt(HEAD_DIM)

    def project_query(rows_ref, target):
        size = rows_ref.shape[0]
        where = pl.ds(pl.multiple_of(target, size), size)

        def q_tile(j, carry):
            got = jnp.dot(rows_ref[...], w_all[j], preferred_element_type=f32)
            got = got.astype(bf16) * bf16(scale)
            q_all[2 * j, where, :] = got[:, :half]
            q_all[2 * j + 1, where, :] = got[:, half:]
            return carry

        lax.fori_loop(0, q_tiles, q_tile, 0)

    def project_key_value(rows_ref, target):
        size = rows_ref.shape[0]
        where = pl.ds(pl.multiple_of(target, size), size)
        got = jnp.dot(rows_ref[...], w_all[q_tiles], preferred_element_type=f32)
        got = got.astype(bf16).astype(f32)
        for part, padded in ((got[:, :half], k_pad), (got[:, half:], v_pad)):
            lane = lax.broadcasted_iota(jnp.int32, part.shape, 1)
            turned = pltpu.roll(part, HEAD_DIM, 1)
            low = lane < HEAD_DIM
            zero = jnp.zeros_like(part)
            forms = (
                jnp.where(low, part, zero),
                jnp.where(low, zero, turned),
                jnp.where(low, turned, zero),
                jnp.where(low, zero, part),
            )
            for f, form in enumerate(forms):
                padded[f, where, :] = form.astype(bf16)

    pairs = q_all.shape[0]
    pairs_per_kv = pairs // (half // HEAD_DIM)

    def heads_copy(t):
        return remote(
            heads.at[t, lo], heads.at[t, lo], hd_s.at[t], hd_r.at[t], section, sibling
        )

    def attend(t, after=None):
        first, keys = t * rows, (t + 1) * rows

        def pair(p, carry):
            query = q_all[p, first : first + rows, :]
            row_at = first + lax.broadcasted_iota(jnp.int32, (rows, keys), 0)
            key_at = lax.broadcasted_iota(jnp.int32, (rows, keys), 1)
            seen = row_at >= key_at
            kv = p // pairs_per_kv
            total = None
            for which in range(2):
                scores = lax.dot_general(
                    query,
                    k_pad[kv * 2 + which, :keys, :],
                    (((1,), (1,)), ((), ())),
                    preferred_element_type=f32,
                )
                scores = jnp.where(seen, scores, -1e30)
                top = jnp.max(scores, axis=-1, keepdims=True)
                weights = jnp.exp(scores - top)
                weights = weights * (1.0 / jnp.sum(weights, axis=-1, keepdims=True))
                term = jnp.dot(
                    weights.astype(bf16),
                    v_pad[kv * 2 + which, :keys, :],
                    preferred_element_type=f32,
                )
                total = term if total is None else total + term
            heads[t, lo, :, pl.ds(pl.multiple_of(p * half, half), half)] = total.astype(bf16)
            if after is not None:
                after(p)
            return carry

        lax.fori_loop(0, pairs, pair, 0)
        heads_copy(t).start()

    def out_dot(t, c):
        got = jnp.dot(heads[t, 0], w_out[0, c], preferred_element_type=f32)
        return got + jnp.dot(heads[t, 1], w_out[1, c], preferred_element_type=f32)

    def cross_copy(j, q):
        return remote(give.at[j, q], x_in.at[j, q], xs_s.at[j, q], xs_r.at[j, q], section, peer)

    def peer_output(t, j, c):
        got = out_dot(t, c).astype(bf16)
        for i in range(per_dot):
            give[j, c * per_dot + i] = got[:, i * cols : (i + 1) * cols]
            cross_copy(j, c * per_dot + i).start()

    def own_output(t, j, c):
        got = out_dot(t, c)
        for i in range(per_dot):
            own_part[j, c * per_dot + i] = got[:, i * cols : (i + 1) * cols]

    def loop(count, body):
        def step(i, carry):
            body(i)
            return carry

        lax.fori_loop(0, count, step, 0)

    def out_copy(j, q):
        return remote(
            mixed.at[j, q],
            out.at[0, :, pl.ds(pl.multiple_of(my_side + q * cols, cols), cols)],
            out_s.at[j, q],
            out_r.at[lo, q],
            nxt,
            hi * 2 + j,
        )

    def hist_arrival(k, i, q):
        place = hist_in.at[k - 1, i, q]
        return remote(
            place, place, hist_s.at[k - 1, 0, q], hist_r.at[k - 1, i, q], section, sibling
        )

    load_mix.wait()
    position = lax.broadcasted_iota(jnp.int32, mix_v.shape, 1)

    def factors_of(s):
        return jnp.sum(jnp.where(position == s, mix_v[...], 0.0), axis=1, keepdims=True)

    factors = factors_of(section)
    plain = jnp.where(section == last, jnp.ones_like(factors[0:1]), factors[0:1])

    def finish(j, q):
        cross_copy(j, q).wait_recv()
        total = own_part[j, q] + x_in[j, q].astype(f32)
        past = x_res[j, :, pl.ds(pl.multiple_of(q * cols, cols), cols)].astype(f32)
        block = (past + total).astype(bf16)
        acc[...] = plain * block.astype(f32)
        for k in range(1, slots + 1):

            @pl.when(gets[k - 1])
            def _():
                hist_arrival(k, j, q).wait_recv()
                acc[...] += factors[k : k + 1] * hist_in[k - 1, j, q].astype(f32)

        mixed[j, q] = acc[...].astype(bf16)
        out_copy(j, q).start()

    def receive_block(j):
        for i in range(UNITS // 2):
            gather_copy(j, i).wait_recv()
            forward_copy(j, i).start()
        for i in range(UNITS // 2):
            forward_copy(j, i).wait_recv()

    for copy in loads:
        copy.wait()
    project_key_value(chip_rows, hi * 2 * rows)
    project_query(chip_rows, hi * 2 * rows)

    def out_weights_ready():
        for copy in out_loads:
            copy.wait()
        for c in range(DOTS):
            weight_copy(c).wait_recv()
        load_res.wait()
        residual_copy().wait_recv()

    def peer_block(j):
        target = ((1 - hi) * 2 + j) * rows
        return peer_rows.at[j], target

    @pl.when(hi == 0)
    def _():
        attend(0)
        attend(1)

    out_weights_ready()

    @pl.when(hi == 0)
    def _():
        for j in range(2):
            heads_copy(j).wait_recv()
            loop(DOTS, lambda c: own_output(j, j, c))

    @pl.when(late)
    def _():
        send_history()

    receive_block(0)
    project_key_value(*peer_block(0))
    project_query(*peer_block(0))

    @pl.when(hi == 0)
    def _():
        attend(2)
        heads_copy(2).wait_recv()
        loop(DOTS, lambda c: peer_output(2, 0, c))

    @pl.when(hi == 1)
    def _():
        attend(0)
        heads_copy(0).wait_recv()
        loop(DOTS, lambda c: peer_output(0, 0, c))

    receive_block(1)
    project_key_value(*peer_block(1))

    @pl.when(hi == 0)
    def _():
        finish(0, 0)

    @pl.when(hi == 1)
    def _():
        attend(2)

    project_query(*peer_block(1))

    @pl.when(hi == 0)
    def _():
        finish(0, 1)

        def after(p):
            @pl.when(p % 3 == 2)
            def _():
                finish(0, 2 + p // 3)

        attend(3, after)
        heads_copy(3).wait_recv()

        def step(c):
            peer_output(3, 1, c)
            finish(0, 4 + c)

        loop(DOTS, step)
        loop(CHUNKS, lambda q: finish(1, q))

    @pl.when(hi == 1)
    def _():
        heads_copy(2).wait_recv()

        def first(c):
            own_output(2, 0, c)
            loop(per_dot, lambda i: finish(0, c * per_dot + i))

        loop(DOTS // 2, first)
        attend(1)
        loop(DOTS // 2, lambda c: first(DOTS // 2 + c))
        heads_copy(1).wait_recv()
        loop(DOTS, lambda c: peer_output(1, 1, c))
        attend(3)
        heads_copy(3).wait_recv()

        def second(c):
            own_output(3, 1, c)
            loop(per_dot, lambda i: finish(1, c * per_dot + i))

        loop(DOTS, second)

    def out_arrival(c, q):
        place = out.at[0, :, pl.ds(pl.multiple_of(c * side + q * cols, cols), cols)]
        return remote(place, place, out_s.at[0, q], out_r.at[c, q], section, sibling)

    late_factors = factors_of(last)

    def take(q):
        for c in range(2):
            out_arrival(c, q).wait_recv()

            @pl.when(section == 0)
            def _():
                where = pl.ds(pl.multiple_of(c * side + q * cols, cols), cols)
                acc[...] = late_factors[0:1] * out[0, :, where].astype(f32)
                for k in range(1, slots + 1):

                    @pl.when(gets_last[k - 1])
                    def _():
                        hist_arrival(k, c, q).wait_recv()
                        acc[...] += late_factors[k : k + 1] * hist_in[k - 1, c, q].astype(f32)

                out[0, :, where] = acc[...].astype(bf16)

    loop(CHUNKS, take)

    for u in range(UNITS):
        sibling_copy(u).wait_send()
    for j in range(2):
        for i in range(UNITS // 2):
            gather_copy(j, i).wait_send()
            forward_copy(j, i).wait_send()
    for c in range(DOTS):
        weight_copy(c).wait_send()
    residual_copy().wait_send()
    for t in range(4):
        heads_copy(t).wait_send()
    for k in range(1, slots + 1):
        for to_last, sends in ((False, gives[k - 1]), (True, gives_last[k - 1])):

            @pl.when(sends)
            def _():
                def each(q, carry):
                    for c in range(2):
                        hist_copy(k, c, q, to_last).wait_send()
                    return carry

                lax.fori_loop(0, CHUNKS, each, 0)

    def drain(q):
        for j in range(2):
            cross_copy(j, q).wait_send()
            out_copy(j, q).wait_send()

    loop(CHUNKS, drain)


def solution(mesh):
    sections, tensor = mesh.shape["section"], mesh.shape["tensor"]
    assert tensor == 4

    def on_device(x, history, wq, wk, wv, wo, mix_weights):
        rows, width = x.shape[1:]
        slots = history.shape[1]
        q_width, kv_width = wq.shape[2], wk.shape[2]
        seq = rows * tensor
        tile = 2 * kv_width
        q_tiles = q_width // tile
        side = width // 2
        wide, cols = side // DOTS, side // CHUNKS
        bf16, f32 = jnp.bfloat16, jnp.float32
        dma = pltpu.SemaphoreType.DMA
        hbm = pl.BlockSpec(memory_space=pltpu.HBM)
        factors = mix_weights.T
        return pl.pallas_call(
            functools.partial(tick_kernel, sections),
            out_shape=pltpu.VMEM(x.shape, bf16),
            in_specs=[hbm] * 7,
            out_specs=pl.BlockSpec(memory_space=pltpu.VMEM),
            scratch_shapes=[
                pltpu.VMEM((rows, width), bf16),
                pltpu.VMEM((2, rows, side), bf16),
                pltpu.VMEM((2 * rows, width), bf16),
                pltpu.VMEM((2, rows, width), bf16),
                pltpu.VMEM((q_tiles + 1, width, tile), bf16),
                pltpu.VMEM((2, DOTS, q_width, wide), bf16),
                pltpu.VMEM((2 * q_tiles, seq, kv_width), bf16),
                pltpu.VMEM((4, seq, kv_width), bf16),
                pltpu.VMEM((4, seq, kv_width), bf16),
                pltpu.VMEM((4, 2, rows, q_width), bf16),
                pltpu.VMEM((2, CHUNKS, rows, cols), f32),
                pltpu.VMEM((2, CHUNKS, rows, cols), bf16),
                pltpu.VMEM((2, CHUNKS, rows, cols), bf16),
                pltpu.VMEM((2, CHUNKS, rows, cols), bf16),
                pltpu.VMEM((rows, cols), f32),
                pltpu.VMEM((slots, 2, CHUNKS, rows, cols), bf16),
                pltpu.VMEM(factors.shape, factors.dtype),
                dma((q_tiles + 2,)),
                dma((DOTS,)),
                dma,
                dma,
                dma,
                dma((slots, 2, CHUNKS)),
                dma((slots, 2, CHUNKS)),
                dma((UNITS,)),
                dma((UNITS,)),
                dma((2, UNITS // 2)),
                dma((2, UNITS // 2)),
                dma((2, UNITS // 2)),
                dma((2, UNITS // 2)),
                dma((DOTS,)),
                dma((DOTS,)),
                dma,
                dma,
                dma((4,)),
                dma((4,)),
                dma((2, CHUNKS)),
                dma((2, CHUNKS)),
                dma((2, CHUNKS)),
                dma((2, CHUNKS)),
            ],
            compiler_params=pltpu.CompilerParams(
                collective_id=0, has_side_effects=True, vmem_limit_bytes=56 * 1024 * 1024
            ),
        )(x, history, wq, wk, wv, wo, factors)

    placed = (
        P("section", "tensor", None),
        P("section", None, "tensor", None),
        P("section", None, "tensor"),
        P("section", None, "tensor"),
        P("section", None, "tensor"),
        P("section", "tensor", None),
        P(),
    )
    return jax.shard_map(
        on_device,
        mesh=mesh,
        in_specs=placed,
        out_specs=P("section", "tensor", None),
        check_vma=False,
    )
```

```python
import functools
import math

import jax
import jax.numpy as jnp
from jax import lax
from jax.experimental import pallas as pl
from jax.experimental.pallas import tpu as pltpu
from jax.sharding import PartitionSpec as P

HEAD_DIM = 64
DILATION_STRIDE = 4
MESH = pl.DeviceIdType.MESH
UNITS = 8
DOTS = 4
CHUNKS = 16
PASTS = 4
PAIR = 2


def start(copy):
    copy.start()
    return copy


def tick_kernel(
    sections,
    x_hbm,
    hist_hbm,
    wq_hbm,
    wk_hbm,
    wv_hbm,
    wo_hbm,
    mix_hbm,
    out,
    x_own,
    x_res,
    chip_rows,
    peer_rows,
    w_all,
    w_out,
    q_all,
    k_pad,
    v_pad,
    heads,
    own_part,
    give,
    x_in,
    mixed,
    acc,
    hist_in,
    mix_v,
    w_sem,
    wo_sem,
    x_sem,
    res_sem,
    mix_sem,
    hist_s,
    hist_r,
    sib_s,
    sib_r,
    gx_s,
    gx_r,
    fw_s,
    fw_r,
    wr_s,
    wr_r,
    xr_s,
    xr_r,
    hd_s,
    hd_r,
    xs_s,
    xs_r,
    out_s,
    out_r,
    near_sem,
    far_sem,
):
    section = lax.axis_index("section")
    me = lax.axis_index("tensor")
    hi, lo = me // 2, me % 2
    sibling = hi * 2 + (1 - lo)
    peer = (1 - hi) * 2 + lo
    rows, width = x_own.shape
    slots = hist_in.shape[0]
    unit = rows // UNITS
    side = width // 2
    wide = side // DOTS
    cols = side // CHUNKS
    per_dot = CHUNKS // DOTS
    past = side // PASTS
    per_past = CHUNKS // PASTS
    q_tiles = w_all.shape[0] - 1
    tile = w_all.shape[2]
    half = tile // 2
    last = sections - 1
    nxt = lax.rem(section + 1, sections)
    prv = lax.rem(section + sections - 1, sections)
    f32, bf16 = jnp.float32, jnp.bfloat16

    middle = (section > 0) & (section < last)
    gets = [middle & (section >= DILATION_STRIDE * k) for k in range(1, slots + 1)]
    gets_last = [(section == 0) & (last >= DILATION_STRIDE * k) for k in range(1, slots + 1)]
    gives = [section + DILATION_STRIDE * k < last for k in range(1, slots + 1)]
    gives_last = [section + DILATION_STRIDE * k == last for k in range(1, slots + 1)]

    def load_unit(i):
        if i < 2:
            at = pl.ds(pl.multiple_of(order[i] * unit, unit), unit)
        else:
            at = pl.ds(2 * unit, rows - 2 * unit)
        return pltpu.make_async_copy(x_hbm.at[0, at], x_own.at[at], x_sem.at[i])

    order = [lo, 1 - lo] + list(range(2, UNITS))
    for i in range(3):
        load_unit(i).start()
    barrier = pltpu.get_barrier_semaphore()

    def greet(s, t):
        pl.semaphore_signal(
            barrier, inc=1, device_id={"section": s, "tensor": t}, device_id_type=MESH
        )

    host = hi == lo
    keeper = hi * 2 + (1 - hi)

    @pl.when(jnp.logical_not(host))
    def _():
        greet(section, sibling)
        greet(section, peer)

    greet(prv, keeper)
    expected = jnp.int32(2)
    for k in range(1, slots + 1):
        step = DILATION_STRIDE * k

        @pl.when(gets[k - 1])
        def _():
            greet(section - step, keeper)

        @pl.when(gets_last[k - 1])
        def _():
            greet(last - step, keeper)

        expected = expected + 2 * (gives[k - 1] | gives_last[k - 1]).astype(jnp.int32)

    loads = [
        pltpu.make_async_copy(
            wk_hbm.at[0], w_all.at[q_tiles, :, pl.ds(0, half)], w_sem
        ),
        pltpu.make_async_copy(
            wv_hbm.at[0], w_all.at[q_tiles, :, pl.ds(half, half)], w_sem
        ),
    ]
    for j in range(q_tiles):
        loads.append(
            pltpu.make_async_copy(
                wq_hbm.at[0, :, pl.ds(j * tile, tile)], w_all.at[j], w_sem
            )
        )
    for copy in loads:
        copy.start()
    load_mix = start(pltpu.make_async_copy(mix_hbm, mix_v, mix_sem))
    mine = pl.multiple_of(lo * rows, rows)
    my_side = pl.multiple_of(lo * side, side)
    other_side = pl.multiple_of((1 - lo) * side, side)

    def norm_unit(u):
        def norm_rows(i, carry):
            at = pl.multiple_of(u * unit + i * 16, 16)
            values = x_own[pl.ds(at, 16), :].astype(f32)
            inv = lax.rsqrt(jnp.mean(values * values, axis=-1, keepdims=True) + 1e-05)
            chip_rows[pl.ds(pl.multiple_of(mine + at, 16), 16), :] = (values * inv).astype(bf16)
            return carry

        lax.fori_loop(0, unit // 16, norm_rows, 0)

    def remote(src, dst, send, recv, s, t):
        return pltpu.make_async_remote_copy(
            src_ref=src,
            dst_ref=dst,
            send_sem=send,
            recv_sem=recv,
            device_id={"section": s, "tensor": t},
            device_id_type=MESH,
        )

    def settle(place, sem):
        return remote(place, place, sem, sem, section, sibling)

    def sibling_copy(u):
        place = chip_rows.at[pl.ds(pl.multiple_of(mine + u * unit, unit), unit)]
        return remote(place, place, sib_s, sib_r.at[u], section, sibling)

    def gather_copy(j, i):
        at = (2 * i + lo) * unit
        return remote(
            chip_rows.at[pl.ds(pl.multiple_of(j * rows + at, unit), unit)],
            peer_rows.at[j, pl.ds(pl.multiple_of(at, unit), unit)],
            gx_s,
            gx_r.at[j, i],
            section,
            peer,
        )

    def forward_copy(j, i):
        place = peer_rows.at[j, pl.ds(pl.multiple_of((2 * i + lo) * unit, unit), unit)]
        return remote(place, place, fw_s, fw_r.at[j], section, sibling)

    def hist_copy(k, c, q, to_last):
        src = hist_hbm.at[0, k - 1, :, pl.ds(pl.multiple_of(c * side + q * past, past), past)]
        slot = c if to_last else lo
        if to_last:
            s, t = 0, me
        else:
            s, t = section + DILATION_STRIDE * k, hi * 2 + c
        return remote(
            src,
            hist_in.at[k - 1, slot, q],
            hist_s.at[k - 1],
            hist_r.at[k - 1, slot, q],
            s,
            t,
        )

    def send_history():
        for k in range(1, slots + 1):
            for to_last, sends in ((False, gives[k - 1]), (True, gives_last[k - 1])):

                @pl.when(sends)
                def _():
                    def each(q, carry):
                        for c in range(2):
                            hist_copy(k, c, q, to_last).start()
                        return carry

                    lax.fori_loop(0, PASTS, each, 0)

    late = (lo == 1) & (section % 2 == 0)

    def tell(sem, t):
        pl.semaphore_signal(
            sem, inc=1, device_id={"section": section, "tensor": t}, device_id_type=MESH
        )

    load_unit(0).wait()
    norm_unit(order[0])

    @pl.when(host)
    def _():
        pl.semaphore_wait(barrier, 2)
        gather_copy(lo, 0).start()
        tell(near_sem, sibling)
        tell(near_sem, peer)
        sibling_copy(order[0]).start()

    load_unit(1).wait()
    norm_unit(order[1])

    @pl.when(jnp.logical_not(host))
    def _():
        pl.semaphore_wait(near_sem, 2)
        gather_copy(lo, 0).start()
        sibling_copy(order[0]).start()

    sibling_copy(order[1]).start()
    load_unit(2).wait()
    for i in range(2, UNITS):
        norm_unit(order[i])
        sibling_copy(order[i]).start()
        if i % 2 == 0:

            @pl.when(lo == 0)
            def _():
                gather_copy(0, i // 2).start()

    @pl.when(lo == 0)
    def _():
        for i in range(UNITS // 2):
            sibling_copy(2 * i).wait_recv()
            gather_copy(1, i).start()
        for i in range(UNITS // 2):
            sibling_copy(2 * i + 1).wait_recv()

    @pl.when(lo == 1)
    def _():
        for i in range(UNITS // 2):
            sibling_copy(2 * i + 1).wait_recv()
            gather_copy(0, i).start()
        for i in range(1, UNITS // 2):
            gather_copy(1, i).start()
        for i in range(UNITS // 2):
            sibling_copy(2 * i).wait_recv()

    @pl.when(jnp.logical_not(host))
    def _():
        pl.semaphore_wait(barrier, expected)
        tell(far_sem, sibling)

    @pl.when(host)
    def _():
        pl.semaphore_wait(far_sem, 1)

    @pl.when(jnp.logical_not(late))
    def _():
        send_history()

    def weight_copy(c):
        return remote(
            wo_hbm.at[0, :, pl.ds(pl.multiple_of(other_side + c * wide, wide), wide)],
            w_out.at[lo, c],
            wr_s,
            wr_r,
            section,
            sibling,
        )

    def residual_copy():
        return remote(
            x_own.at[:, pl.ds(other_side, side)], x_res.at[lo], xr_s, xr_r, section, sibling
        )

    for c in range(DOTS):
        pltpu.make_async_copy(
            wo_hbm.at[0, :, pl.ds(pl.multiple_of(my_side + c * wide, wide), wide)],
            w_out.at[lo, c],
            wo_sem,
        ).start()
        weight_copy(c).start()
    load_res = start(
        pltpu.make_async_copy(x_hbm.at[0, :, pl.ds(my_side, side)], x_res.at[lo], res_sem)
    )
    residual_copy().start()

    scale = 1.0 / math.sqrt(HEAD_DIM)

    def project_query(rows_ref, target, begin=0, end=None):
        size = rows_ref.shape[0]
        where = pl.ds(pl.multiple_of(target, size), size)

        def q_tile(j, carry):
            got = jnp.dot(rows_ref[...], w_all[j], preferred_element_type=f32)
            got = got.astype(bf16) * bf16(scale)
            q_all[2 * j, where, :] = got[:, :half]
            q_all[2 * j + 1, where, :] = got[:, half:]
            return carry

        lax.fori_loop(begin, q_tiles if end is None else end, q_tile, 0)

    def project_key_value(rows_ref, target):
        size = rows_ref.shape[0]
        where = pl.ds(pl.multiple_of(target, size), size)
        got = jnp.dot(rows_ref[...], w_all[q_tiles], preferred_element_type=f32)
        got = got.astype(bf16).astype(f32)
        for part, padded in ((got[:, :half], k_pad), (got[:, half:], v_pad)):
            lane = lax.broadcasted_iota(jnp.int32, part.shape, 1)
            turned = pltpu.roll(part, HEAD_DIM, 1)
            low = lane < HEAD_DIM
            zero = jnp.zeros_like(part)
            forms = (
                jnp.where(low, part, zero),
                jnp.where(low, zero, turned),
                jnp.where(low, turned, zero),
                jnp.where(low, zero, part),
            )
            for f, form in enumerate(forms):
                padded[f, where, :] = form.astype(bf16)

    pairs = q_all.shape[0]
    pairs_per_kv = pairs // (half // HEAD_DIM)

    def heads_copy(t):
        return remote(
            heads.at[t, lo], heads.at[t, lo], hd_s, hd_r.at[t], section, sibling
        )

    def attend(t, after=None):
        first, keys = t * rows, (t + 1) * rows
        seen = lax.broadcasted_iota(jnp.int32, (rows, rows), 0) >= lax.broadcasted_iota(
            jnp.int32, (rows, rows), 1
        )

        def group(kv, carry):
            chains = [(i, which) for i in range(pairs_per_kv) for which in range(2)]
            scores = []
            for i, which in chains:
                got = lax.dot_general(
                    q_all[kv * pairs_per_kv + i, first:keys, :],
                    k_pad[kv * 2 + which, :keys, :],
                    (((1,), (1,)), ((), ())),
                    preferred_element_type=f32,
                )
                scores.append((got[:, :first], jnp.where(seen, got[:, first:], -1e30)))
            probs = []
            for before, here in scores:
                top = jnp.max(here, axis=-1, keepdims=True)
                if first:
                    top = jnp.maximum(top, jnp.max(before, axis=-1, keepdims=True))
                here = jnp.exp(here - top)
                norm = jnp.sum(here, axis=-1, keepdims=True)
                if first:
                    before = jnp.exp(before - top)
                    norm = norm + jnp.sum(before, axis=-1, keepdims=True)
                inv = 1.0 / norm
                parts = [(here * inv).astype(bf16)]
                if first:
                    parts.insert(0, (before * inv).astype(bf16))
                probs.append(jnp.concatenate(parts, axis=1) if first else parts[0])
            terms = [
                jnp.dot(weights, v_pad[kv * 2 + which, :keys, :], preferred_element_type=f32)
                for weights, (i, which) in zip(probs, chains)
            ]
            for i in range(pairs_per_kv):
                total = terms[2 * i] + terms[2 * i + 1]
                at = pl.multiple_of((kv * pairs_per_kv + i) * half, half)
                heads[t, lo, :, pl.ds(at, half)] = total.astype(bf16)
            if after is not None:
                after(kv)
            return carry

        lax.fori_loop(0, pairs // pairs_per_kv, group, 0)
        heads_copy(t).start()

    def out_dot(t, c):
        got = jnp.dot(heads[t, 0], w_out[0, c], preferred_element_type=f32)
        return got + jnp.dot(heads[t, 1], w_out[1, c], preferred_element_type=f32)

    def cross_copy(j, q):
        span = PAIR if j == 0 else 1
        place = pl.ds(q, span)
        return remote(
            give.at[j, place], x_in.at[j, place], xs_s, xs_r.at[j, q], section, peer
        )

    def peer_output(t, j, c):
        got = out_dot(t, c).astype(bf16)
        span = PAIR if j == 0 else 1
        for i in range(per_dot):
            give[j, c * per_dot + i] = got[:, i * cols : (i + 1) * cols]
            if i % span == span - 1:
                cross_copy(j, c * per_dot + i - (span - 1)).start()

    def own_output(t, j, c):
        got = out_dot(t, c)
        for i in range(per_dot):
            own_part[j, c * per_dot + i] = got[:, i * cols : (i + 1) * cols]

    def loop(count, body):
        def step(i, carry):
            body(i)
            return carry

        lax.fori_loop(0, count, step, 0)

    def out_copy(j, q):
        return remote(
            mixed.at[j, q],
            out.at[0, :, pl.ds(pl.multiple_of(my_side + q * cols, cols), cols)],
            out_s,
            out_r.at[lo, q // PAIR],
            nxt,
            hi * 2 + j,
        )

    def hist_arrival(k, i, q):
        place = hist_in.at[k - 1, i, q]
        return remote(
            place, place, hist_s.at[k - 1], hist_r.at[k - 1, i, q], section, sibling
        )

    def history_of(k, i, q):
        @pl.when(q % per_past == 0)
        def _():
            hist_arrival(k, i, q // per_past).wait_recv()

        where = pl.ds(pl.multiple_of((q % per_past) * cols, cols), cols)
        return hist_in[k - 1, i, q // per_past, :, where].astype(f32)

    load_mix.wait()
    position = lax.broadcasted_iota(jnp.int32, mix_v.shape, 1)

    def factors_of(s):
        return jnp.sum(jnp.where(position == s, mix_v[...], 0.0), axis=1, keepdims=True)

    factors = factors_of(section)
    plain = jnp.where(section == last, jnp.ones_like(factors[0:1]), factors[0:1])

    def finish(j, q):
        if j == 0:

            @pl.when(q % PAIR == 0)
            def _():
                cross_copy(j, q).wait_recv()

        else:
            cross_copy(j, q).wait_recv()
        total = own_part[j, q] + x_in[j, q].astype(f32)
        given = x_res[j, :, pl.ds(pl.multiple_of(q * cols, cols), cols)].astype(f32)
        block = (given + total).astype(bf16)
        acc[...] = plain * block.astype(f32)
        for k in range(1, slots + 1):

            @pl.when(gets[k - 1])
            def _():
                acc[...] += factors[k : k + 1] * history_of(k, j, q)

        mixed[j, q] = acc[...].astype(bf16)
        out_copy(j, q).start()

    def receive_block(j, then=None):
        for i in range(UNITS // 2):
            gather_copy(j, i).wait_recv()
            forward_copy(j, i).start()
        if then is not None:
            then()
        settle(peer_rows.at[j, pl.ds(0, rows // 2)], fw_r.at[j]).wait_recv()

    pltpu.make_async_copy(w_all, w_all, w_sem).wait()
    project_key_value(chip_rows, hi * 2 * rows)
    project_query(chip_rows, hi * 2 * rows)

    def out_weights_ready():
        pltpu.make_async_copy(w_out.at[lo], w_out.at[lo], wo_sem).wait()
        settle(w_out.at[1 - lo], wr_r).wait_recv()
        load_res.wait()
        residual_copy().wait_recv()

    def peer_block(j):
        target = ((1 - hi) * 2 + j) * rows
        return peer_rows.at[j], target

    @pl.when(hi == 0)
    def _():
        attend(0)
        attend(1)

    out_weights_ready()

    @pl.when(hi == 0)
    def _():
        for j in range(2):
            heads_copy(j).wait_recv()
            loop(DOTS, lambda c: own_output(j, j, c))

    receive_block(0)
    project_key_value(*peer_block(0))
    project_query(*peer_block(0))

    @pl.when(hi == 0)
    def _():
        attend(2)
        heads_copy(2).wait_recv()
        loop(DOTS, lambda c: peer_output(2, 0, c))

    @pl.when(hi == 1)
    def _():
        attend(0)
        heads_copy(0).wait_recv()
        loop(DOTS, lambda c: peer_output(0, 0, c))

    @pl.when(late)
    def _():
        send_history()

    def finish_part(j, c, parts=2):
        count = CHUNKS // (parts * DOTS)
        loop(count, lambda i: finish(j, c * count + i))

    def first_part():
        @pl.when(hi == 0)
        def _():
            finish_part(0, 0)

    receive_block(1, first_part)
    project_key_value(*peer_block(1))

    @pl.when(hi == 1)
    def _():
        attend(2)

    project_query(*peer_block(1))

    @pl.when(hi == 0)
    def _():
        finish_part(0, 1)
        attend(3, lambda kv: finish_part(0, 2 + kv))
        finish_part(0, 4)
        heads_copy(3).wait_recv()

        def step(c):
            peer_output(3, 1, c)

            @pl.when(c > 0)
            def _():
                finish_part(0, 4 + c)

        loop(DOTS, step)
        loop(CHUNKS, lambda q: finish(1, q))

    @pl.when(hi == 1)
    def _():
        heads_copy(2).wait_recv()
        own_output(2, 0, 0)
        finish_part(0, 0, 1)
        attend(1)
        own_output(2, 0, 1)
        finish_part(0, 1, 1)
        heads_copy(1).wait_recv()

        def first(c):
            peer_output(1, 1, c)

            @pl.when(c < DOTS - 2)
            def _():
                own_output(2, 0, 2 + c)
                finish_part(0, 2 + c, 1)

        loop(DOTS, first)
        attend(3)
        heads_copy(3).wait_recv()

        def second(c):
            own_output(3, 1, c)
            finish_part(1, c, 1)

        loop(DOTS, second)

    def out_arrival(c, q):
        span = PAIR * cols
        place = out.at[0, :, pl.ds(pl.multiple_of(c * side + q * span, span), span)]
        return settle(place, out_r.at[c, q])

    late_factors = factors_of(last)

    def take(q):
        for c in range(2):
            out_arrival(c, q).wait_recv()

            @pl.when(section == 0)
            def _():
                for i in range(PAIR):
                    at = q * PAIR + i
                    where = pl.ds(pl.multiple_of(c * side + at * cols, cols), cols)
                    acc[...] = late_factors[0:1] * out[0, :, where].astype(f32)
                    for k in range(1, slots + 1):

                        @pl.when(gets_last[k - 1])
                        def _():
                            acc[...] += late_factors[k : k + 1] * history_of(k, c, at)

                    out[0, :, where] = acc[...].astype(bf16)

    loop(CHUNKS // PAIR, take)

    settle(chip_rows.at[pl.ds(0, rows)], sib_s).wait_send()
    settle(peer_rows.at[0], gx_s).wait_send()
    settle(peer_rows.at[0], fw_s).wait_send()
    settle(w_out.at[lo], wr_s).wait_send()
    residual_copy().wait_send()
    settle(heads.at[:, lo], hd_s).wait_send()
    for k in range(1, slots + 1):

        @pl.when(gives[k - 1] | gives_last[k - 1])
        def _():
            settle(hist_in.at[k - 1], hist_s.at[k - 1]).wait_send()

    settle(give, xs_s).wait_send()
    settle(mixed, out_s).wait_send()


def solution(mesh):
    sections, tensor = mesh.shape["section"], mesh.shape["tensor"]
    assert tensor == 4

    def on_device(x, history, wq, wk, wv, wo, mix_weights):
        rows, width = x.shape[1:]
        slots = history.shape[1]
        q_width, kv_width = wq.shape[2], wk.shape[2]
        seq = rows * tensor
        tile = 2 * kv_width
        q_tiles = q_width // tile
        side = width // 2
        wide, cols = side // DOTS, side // CHUNKS
        bf16, f32 = jnp.bfloat16, jnp.float32
        dma = pltpu.SemaphoreType.DMA
        hbm = pl.BlockSpec(memory_space=pltpu.HBM)
        factors = mix_weights.T
        return pl.pallas_call(
            functools.partial(tick_kernel, sections),
            out_shape=pltpu.VMEM(x.shape, bf16),
            in_specs=[hbm] * 7,
            out_specs=pl.BlockSpec(memory_space=pltpu.VMEM),
            scratch_shapes=[
                pltpu.VMEM((rows, width), bf16),
                pltpu.VMEM((2, rows, side), bf16),
                pltpu.VMEM((2 * rows, width), bf16),
                pltpu.VMEM((2, rows, width), bf16),
                pltpu.VMEM((q_tiles + 1, width, tile), bf16),
                pltpu.VMEM((2, DOTS, q_width, wide), bf16),
                pltpu.VMEM((2 * q_tiles, seq, kv_width), bf16),
                pltpu.VMEM((4, seq, kv_width), bf16),
                pltpu.VMEM((4, seq, kv_width), bf16),
                pltpu.VMEM((4, 2, rows, q_width), bf16),
                pltpu.VMEM((2, CHUNKS, rows, cols), f32),
                pltpu.VMEM((2, CHUNKS, rows, cols), bf16),
                pltpu.VMEM((2, CHUNKS, rows, cols), bf16),
                pltpu.VMEM((2, CHUNKS, rows, cols), bf16),
                pltpu.VMEM((rows, cols), f32),
                pltpu.VMEM((slots, 2, PASTS, rows, side // PASTS), bf16),
                pltpu.VMEM(factors.shape, factors.dtype),
                dma,
                dma,
                dma((3,)),
                dma,
                dma,
                dma((slots,)),
                dma((slots, 2, PASTS)),
                dma,
                dma((UNITS,)),
                dma,
                dma((2, UNITS // 2)),
                dma,
                dma((2,)),
                dma,
                dma,
                dma,
                dma,
                dma,
                dma((4,)),
                dma,
                dma((2, CHUNKS)),
                dma,
                dma((2, CHUNKS // PAIR)),
                pltpu.SemaphoreType.REGULAR,
                pltpu.SemaphoreType.REGULAR,
            ],
            compiler_params=pltpu.CompilerParams(
                collective_id=0, has_side_effects=True, vmem_limit_bytes=56 * 1024 * 1024
            ),
        )(x, history, wq, wk, wv, wo, factors)

    placed = (
        P("section", "tensor", None),
        P("section", None, "tensor", None),
        P("section", None, "tensor"),
        P("section", None, "tensor"),
        P("section", None, "tensor"),
        P("section", "tensor", None),
        P(),
    )
    return jax.shard_map(
        on_device,
        mesh=mesh,
        in_specs=placed,
        out_specs=P("section", "tensor", None),
        check_vma=False,
    )
```

```python
import functools
import math

import jax
import jax.numpy as jnp
from jax import lax
from jax.experimental import pallas as pl
from jax.experimental.pallas import tpu as pltpu
from jax.sharding import PartitionSpec as P

HEAD_DIM = 64
DILATION_STRIDE = 4
MESH = pl.DeviceIdType.MESH
UNITS = 8
DOTS = 4
CHUNKS = 16
PASTS = 4
PAIR = 2


def start(copy):
    copy.start()
    return copy


def tick_kernel(
    sections,
    x_hbm,
    hist_hbm,
    wq_hbm,
    wk_hbm,
    wv_hbm,
    wo_hbm,
    mix_hbm,
    out,
    x_own,
    x_res,
    chip_rows,
    peer_rows,
    w_all,
    w_out,
    q_all,
    k_pad,
    v_pad,
    heads,
    own_part,
    give,
    x_in,
    mixed,
    acc,
    hist_in,
    mix_v,
    w_sem,
    wo_sem,
    x_sem,
    res_sem,
    mix_sem,
    hist_s,
    hist_r,
    sib_s,
    sib_r,
    gx_s,
    gx_r,
    fw_s,
    fw_r,
    wr_s,
    wr_r,
    xr_s,
    xr_r,
    hd_s,
    hd_r,
    xs_s,
    xs_r,
    out_s,
    out_r,
    near_sem,
    far_sem,
    clear_sem,
):
    section = lax.axis_index("section")
    me = lax.axis_index("tensor")
    hi, lo = me // 2, me % 2
    sibling = hi * 2 + (1 - lo)
    peer = (1 - hi) * 2 + lo
    rows, width = x_own.shape
    slots = hist_in.shape[0]
    unit = rows // UNITS
    side = width // 2
    wide = side // DOTS
    cols = side // CHUNKS
    per_dot = CHUNKS // DOTS
    past = side // PASTS
    per_past = CHUNKS // PASTS
    q_tiles = w_all.shape[0] - 1
    tile = w_all.shape[2]
    half = tile // 2
    last = sections - 1
    nxt = lax.rem(section + 1, sections)
    prv = lax.rem(section + sections - 1, sections)
    f32, bf16 = jnp.float32, jnp.bfloat16

    middle = (section > 0) & (section < last)
    gets = [middle & (section >= DILATION_STRIDE * k) for k in range(1, slots + 1)]
    gets_last = [(section == 0) & (last >= DILATION_STRIDE * k) for k in range(1, slots + 1)]
    gives = [section + DILATION_STRIDE * k < last for k in range(1, slots + 1)]
    gives_last = [section + DILATION_STRIDE * k == last for k in range(1, slots + 1)]

    def load_unit(i):
        if i < 2:
            at = pl.ds(pl.multiple_of(order[i] * unit, unit), unit)
        else:
            at = pl.ds(2 * unit, rows - 2 * unit)
        return pltpu.make_async_copy(x_hbm.at[0, at], x_own.at[at], x_sem.at[i])

    order = [lo, 1 - lo] + list(range(2, UNITS))
    for i in range(3):
        load_unit(i).start()
    barrier = pltpu.get_barrier_semaphore()

    def greet(s, t):
        pl.semaphore_signal(
            barrier, inc=1, device_id={"section": s, "tensor": t}, device_id_type=MESH
        )

    host = hi == lo
    keeper = hi * 2 + (1 - hi)

    @pl.when(jnp.logical_not(host))
    def _():
        greet(section, sibling)
        greet(section, peer)

    greet(prv, keeper)
    expected = jnp.int32(2)
    for k in range(1, slots + 1):
        step = DILATION_STRIDE * k

        @pl.when(gets[k - 1])
        def _():
            greet(section - step, keeper)

        @pl.when(gets_last[k - 1])
        def _():
            greet(last - step, keeper)

        expected = expected + 2 * (gives[k - 1] | gives_last[k - 1]).astype(jnp.int32)

    loads = [
        pltpu.make_async_copy(
            wk_hbm.at[0], w_all.at[q_tiles, :, pl.ds(0, half)], w_sem
        ),
        pltpu.make_async_copy(
            wv_hbm.at[0], w_all.at[q_tiles, :, pl.ds(half, half)], w_sem
        ),
    ]
    for j in range(q_tiles):
        loads.append(
            pltpu.make_async_copy(
                wq_hbm.at[0, :, pl.ds(j * tile, tile)], w_all.at[j], w_sem
            )
        )
    for copy in loads:
        copy.start()
    load_mix = start(pltpu.make_async_copy(mix_hbm, mix_v, mix_sem))
    mine = pl.multiple_of(lo * rows, rows)
    my_side = pl.multiple_of(lo * side, side)
    other_side = pl.multiple_of((1 - lo) * side, side)

    def norm_unit(u):
        def norm_rows(i, carry):
            at = pl.multiple_of(u * unit + i * 16, 16)
            values = x_own[pl.ds(at, 16), :].astype(f32)
            inv = lax.rsqrt(jnp.mean(values * values, axis=-1, keepdims=True) + 1e-05)
            chip_rows[pl.ds(pl.multiple_of(mine + at, 16), 16), :] = (values * inv).astype(bf16)
            return carry

        lax.fori_loop(0, unit // 16, norm_rows, 0)

    def remote(src, dst, send, recv, s, t):
        return pltpu.make_async_remote_copy(
            src_ref=src,
            dst_ref=dst,
            send_sem=send,
            recv_sem=recv,
            device_id={"section": s, "tensor": t},
            device_id_type=MESH,
        )

    def settle(place, sem):
        return remote(place, place, sem, sem, section, sibling)

    def sibling_copy(u):
        place = chip_rows.at[pl.ds(pl.multiple_of(mine + u * unit, unit), unit)]
        return remote(place, place, sib_s, sib_r, section, sibling)

    share = UNITS // 2

    def unit_of(i):
        return UNITS - 2 if i == share else 2 * i + lo

    def gather_copy(j, i):
        at = unit_of(i) * unit
        return remote(
            chip_rows.at[pl.ds(pl.multiple_of(j * rows + at, unit), unit)],
            peer_rows.at[j, pl.ds(pl.multiple_of(at, unit), unit)],
            gx_s,
            gx_r.at[j, i],
            section,
            peer,
        )

    def forward_copy(j, i):
        place = peer_rows.at[j, pl.ds(pl.multiple_of(unit_of(i) * unit, unit), unit)]
        return remote(place, place, fw_s, fw_r.at[j], section, sibling)

    def hist_copy(k, c, q, to_last):
        src = hist_hbm.at[0, k - 1, :, pl.ds(pl.multiple_of(c * side + q * past, past), past)]
        slot = c if to_last else lo
        if to_last:
            s, t = 0, me
        else:
            s, t = section + DILATION_STRIDE * k, hi * 2 + c
        return remote(
            src,
            hist_in.at[k - 1, slot, q],
            hist_s.at[k - 1],
            hist_r.at[k - 1, slot, q],
            s,
            t,
        )

    def send_history():
        for k in range(1, slots + 1):
            for to_last, sends in ((False, gives[k - 1]), (True, gives_last[k - 1])):

                @pl.when(sends)
                def _():
                    def each(q, carry):
                        for c in range(2):
                            hist_copy(k, c, q, to_last).start()
                        return carry

                    lax.fori_loop(0, PASTS, each, 0)

    late = (lo == 1) & (section % 2 == 0)

    def tell(sem, t):
        pl.semaphore_signal(
            sem, inc=1, device_id={"section": section, "tensor": t}, device_id_type=MESH
        )

    load_unit(0).wait()
    norm_unit(order[0])

    @pl.when(host)
    def _():
        pl.semaphore_wait(barrier, 2)
        gather_copy(lo, 0).start()
        tell(near_sem, sibling)
        tell(near_sem, peer)
        sibling_copy(order[0]).start()

    load_unit(1).wait()
    norm_unit(order[1])

    @pl.when(jnp.logical_not(host))
    def _():
        pl.semaphore_wait(near_sem, 2)
        gather_copy(lo, 0).start()
        sibling_copy(order[0]).start()

    sibling_copy(order[1]).start()
    load_unit(2).wait()
    for i in range(2, UNITS):
        norm_unit(order[i])
        sibling_copy(order[i]).start()
        if i % 2 == 0:

            @pl.when(lo == 0)
            def _():
                gather_copy(0, i // 2).start()

    settle(chip_rows.at[pl.ds(0, rows)], sib_r).wait_recv()

    @pl.when(lo == 0)
    def _():
        for i in range(share - 1):
            gather_copy(1, i).start()

        @pl.when(hi == 1)
        def _():
            gather_copy(1, share - 1).start()

    @pl.when(lo == 1)
    def _():
        for i in range(share):
            gather_copy(0, i).start()
        for i in range(1, share - 1):
            gather_copy(1, i).start()

        @pl.when(hi == 0)
        def _():
            gather_copy(1, share).start()

        gather_copy(1, share - 1).start()

    @pl.when(jnp.logical_not(host))
    def _():
        pl.semaphore_wait(barrier, expected)
        tell(far_sem, sibling)

    @pl.when(host)
    def _():
        pl.semaphore_wait(far_sem, 1)

    @pl.when(jnp.logical_not(late))
    def _():
        send_history()

    def weight_copy(c):
        return remote(
            wo_hbm.at[0, :, pl.ds(pl.multiple_of(other_side + c * wide, wide), wide)],
            w_out.at[lo, c],
            wr_s,
            wr_r,
            section,
            sibling,
        )

    def residual_copy():
        return remote(
            x_own.at[:, pl.ds(other_side, side)], x_res.at[lo], xr_s, xr_r, section, sibling
        )

    for c in range(DOTS):
        pltpu.make_async_copy(
            wo_hbm.at[0, :, pl.ds(pl.multiple_of(my_side + c * wide, wide), wide)],
            w_out.at[lo, c],
            wo_sem,
        ).start()
        weight_copy(c).start()
    load_res = start(
        pltpu.make_async_copy(x_hbm.at[0, :, pl.ds(my_side, side)], x_res.at[lo], res_sem)
    )
    residual_copy().start()

    scale = 1.0 / math.sqrt(HEAD_DIM)

    def project_query(rows_ref, target, begin=0, end=None):
        size = rows_ref.shape[0]
        where = pl.ds(pl.multiple_of(target, size), size)

        def q_tile(j, carry):
            got = jnp.dot(rows_ref[...], w_all[j], preferred_element_type=f32)
            got = got.astype(bf16) * bf16(scale)
            q_all[2 * j, where, :] = got[:, :half]
            q_all[2 * j + 1, where, :] = got[:, half:]
            return carry

        lax.fori_loop(begin, q_tiles if end is None else end, q_tile, 0)

    def project_key_value(rows_ref, first):
        size = rows_ref.shape[0]
        got = jnp.dot(rows_ref[...], w_all[q_tiles], preferred_element_type=f32)
        got = got.astype(bf16).astype(f32)
        for part, padded in ((got[:, :half], k_pad), (got[:, half:], v_pad)):
            lane = lax.broadcasted_iota(jnp.int32, part.shape, 1)
            turned = pltpu.roll(part, HEAD_DIM, 1)
            low = lane < HEAD_DIM
            zero = jnp.zeros_like(part)
            forms = (
                jnp.where(low, part, zero),
                jnp.where(low, zero, turned),
                jnp.where(low, turned, zero),
                jnp.where(low, zero, part),
            )
            for f, form in enumerate(forms):
                for i in range(size // rows):
                    some = form[i * rows : (i + 1) * rows].astype(bf16)
                    padded[f // 2, first + i, f % 2, :, :half] = some

    def fill_ones():
        low = lax.broadcasted_iota(jnp.int32, (rows, half), 1) < HEAD_DIM
        for which in range(2):
            ones = jnp.where(low == (which == 0), 1.0, 0.0).astype(bf16)
            for kv in range(v_pad.shape[0]):
                for i in range(v_pad.shape[1]):
                    v_pad[kv, i, which, :, half:] = ones

    pairs = q_all.shape[0]
    pairs_per_kv = pairs // (half // HEAD_DIM)

    def heads_copy(t, kv):
        span = pairs_per_kv * half
        place = heads.at[t, lo, :, pl.ds(pl.multiple_of(kv * span, span), span)]
        return remote(place, place, hd_s, hd_r.at[t], section, sibling)

    def heads_ready(t):
        settle(heads.at[t, 1 - lo], hd_r.at[t]).wait_recv()

    def attend(t, after=None):
        first, blocks = t * rows, t + 1
        seen = lax.broadcasted_iota(jnp.int32, (rows, rows), 0) >= lax.broadcasted_iota(
            jnp.int32, (rows, rows), 1
        )

        def exponents(scores, which):
            mine = [
                scores[:, (2 * i + which) * rows : (2 * i + which + 1) * rows]
                for i in range(blocks)
            ]
            mine[t] = jnp.where(seen, mine[t], -1e30)
            top = jnp.max(functools.reduce(jnp.maximum, mine), axis=-1, keepdims=True)
            return [jnp.exp(part - top).astype(bf16) for part in mine]

        def group(kv, carry):
            keys = k_pad[kv, :blocks].reshape(2 * blocks * rows, half)
            values = v_pad[kv, :blocks].reshape(2 * blocks * rows, 2 * half)
            scores = [
                lax.dot_general(
                    q_all[kv * pairs_per_kv + i, first : first + rows, :],
                    keys,
                    (((1,), (1,)), ((), ())),
                    preferred_element_type=f32,
                )
                for i in range(pairs_per_kv)
            ]
            probs = []
            for got in scores:
                even, odd = exponents(got, 0), exponents(got, 1)
                both = [part for pair in zip(even, odd) for part in pair]
                probs.append(jnp.concatenate(both, axis=1))
            for i, weights in enumerate(probs):
                both = jnp.dot(weights, values, preferred_element_type=f32)
                total = both[:, :half] / both[:, half:]
                at = pl.multiple_of((kv * pairs_per_kv + i) * half, half)
                heads[t, lo, :, pl.ds(at, half)] = total.astype(bf16)
            heads_copy(t, kv).start()
            if after is not None:
                after(kv)
            return carry

        lax.fori_loop(0, pairs // pairs_per_kv, group, 0)

    def out_dot(t, c):
        got = jnp.dot(heads[t, 0], w_out[0, c], preferred_element_type=f32)
        return got + jnp.dot(heads[t, 1], w_out[1, c], preferred_element_type=f32)

    def cross_copy(j, q):
        return remote(give.at[j, q], x_in.at[j, q], xs_s, xs_r.at[j, q], section, peer)

    def peer_output(t, j, c, send=True):
        got = out_dot(t, c).astype(bf16)
        for i in range(per_dot):
            give[j, c * per_dot + i] = got[:, i * cols : (i + 1) * cols]
            if send:
                cross_copy(j, c * per_dot + i).start()

    def own_output(t, j, c):
        got = out_dot(t, c)
        for i in range(per_dot):
            own_part[j, c * per_dot + i] = got[:, i * cols : (i + 1) * cols]

    def loop(count, body):
        def step(i, carry):
            body(i)
            return carry

        lax.fori_loop(0, count, step, 0)

    def out_copy(j, q):
        return remote(
            mixed.at[j, q],
            out.at[0, :, pl.ds(pl.multiple_of(my_side + q * cols, cols), cols)],
            out_s,
            out_r.at[lo, q // PAIR],
            nxt,
            hi * 2 + j,
        )

    def hist_arrival(k, i, q):
        place = hist_in.at[k - 1, i, q]
        return remote(
            place, place, hist_s.at[k - 1], hist_r.at[k - 1, i, q], section, sibling
        )

    def history_of(k, i, q):
        @pl.when(q % per_past == 0)
        def _():
            hist_arrival(k, i, q // per_past).wait_recv()

        where = pl.ds(pl.multiple_of((q % per_past) * cols, cols), cols)
        return hist_in[k - 1, i, q // per_past, :, where].astype(f32)

    load_mix.wait()
    position = lax.broadcasted_iota(jnp.int32, mix_v.shape, 1)

    def factors_of(s):
        return jnp.sum(jnp.where(position == s, mix_v[...], 0.0), axis=1, keepdims=True)

    factors = factors_of(section)
    plain = jnp.where(section == last, jnp.ones_like(factors[0:1]), factors[0:1])

    def finish(j, q):
        cross_copy(j, q).wait_recv()
        total = own_part[j, q] + x_in[j, q].astype(f32)
        given = x_res[j, :, pl.ds(pl.multiple_of(q * cols, cols), cols)].astype(f32)
        block = (given + total).astype(bf16)
        acc[...] = plain * block.astype(f32)
        for k in range(1, slots + 1):

            @pl.when(gets[k - 1])
            def _():
                acc[...] += factors[k : k + 1] * history_of(k, j, q)

        mixed[j, q] = acc[...].astype(bf16)
        out_copy(j, q).start()

    def receive_block(j, then=None):
        def pass_on(i):
            gather_copy(j, i).wait_recv()
            forward_copy(j, i).start()

        def passed(count):
            settle(peer_rows.at[j, pl.ds(0, count * unit)], fw_r.at[j]).wait_recv()

        if j == 0:
            for i in range(share):
                pass_on(i)
            passed(share)
            return
        for i in range(share - 1):
            pass_on(i)

        @pl.when((hi == 1) & (lo == 1))
        def _():
            pass_on(share)

        @pl.when((hi == 0) | (lo == 1))
        def _():
            pass_on(share - 1)

        then()

        @pl.when(hi == 0)
        def _():
            passed(share)

        @pl.when((hi == 1) & (lo == 0))
        def _():
            passed(share + 1)

        @pl.when((hi == 1) & (lo == 1))
        def _():
            passed(share - 1)

    fill_ones()
    pltpu.make_async_copy(w_all, w_all, w_sem).wait()
    project_key_value(chip_rows, hi * 2)
    project_query(chip_rows, hi * 2 * rows)

    def out_weights_ready():
        pltpu.make_async_copy(w_out.at[lo], w_out.at[lo], wo_sem).wait()
        settle(w_out.at[1 - lo], wr_r).wait_recv()
        load_res.wait()
        residual_copy().wait_recv()

    def peer_block(j):
        target = ((1 - hi) * 2 + j) * rows
        return peer_rows.at[j], target

    @pl.when(hi == 0)
    def _():
        attend(0)
        attend(1)

    out_weights_ready()

    @pl.when(hi == 0)
    def _():
        for j in range(2):
            heads_ready(j)
            loop(DOTS, lambda c: own_output(j, j, c))

    receive_block(0)
    project_key_value(peer_rows.at[0], (1 - hi) * 2)
    project_query(*peer_block(0))

    @pl.when(hi == 0)
    def _():
        attend(2)

        @pl.when(jnp.logical_not(host))
        def _():
            settle(peer_rows.at[0], gx_s).wait_send()
            settle(peer_rows.at[0, pl.ds(0, unit)], gx_s).wait_send()
            tell(clear_sem, sibling)
            heads_ready(2)
            loop(DOTS, lambda c: peer_output(2, 0, c))

        @pl.when(host)
        def _():
            heads_ready(2)
            loop(DOTS, lambda c: peer_output(2, 0, c, False))
            settle(peer_rows.at[0, pl.ds(0, rows - unit)], gx_s).wait_send()
            pl.semaphore_wait(clear_sem, 1)
            loop(CHUNKS, lambda q: cross_copy(0, q).start())


    @pl.when(hi == 1)
    def _():
        attend(0)
        heads_ready(0)
        loop(DOTS, lambda c: peer_output(0, 0, c))

    @pl.when(late)
    def _():
        send_history()

    def finish_part(j, c, parts=2):
        count = CHUNKS // (parts * DOTS)
        loop(count, lambda i: finish(j, c * count + i))

    def first_part():
        @pl.when(hi == 0)
        def _():
            finish_part(0, 0)

    receive_block(1, first_part)
    project_key_value(peer_rows.at[1], (1 - hi) * 2 + 1)

    @pl.when(hi == 0)
    def _():
        project_query(*peer_block(1))
        finish_part(0, 1)
        attend(3, lambda kv: finish_part(0, 2 + kv))
        finish_part(0, 4)
        heads_ready(3)

        def step(c):
            peer_output(3, 1, c)

            @pl.when(c > 0)
            def _():
                finish_part(0, 4 + c)

        loop(DOTS, step)
        loop(CHUNKS, lambda q: finish(1, q))

    @pl.when(hi == 1)
    def _():
        attend(2)
        project_query(*peer_block(1), 0, q_tiles - 1)
        heads_ready(2)
        own_output(2, 0, 0)
        finish_part(0, 0, 1)
        project_query(*peer_block(1), q_tiles - 1, q_tiles)
        attend(1)
        own_output(2, 0, 1)
        finish_part(0, 1, 1)
        heads_ready(1)

        def first(c):
            peer_output(1, 1, c)

            @pl.when(c < DOTS - 2)
            def _():
                own_output(2, 0, 2 + c)
                finish_part(0, 2 + c, 1)

        loop(DOTS, first)
        attend(3)
        heads_ready(3)

        def second(c):
            own_output(3, 1, c)
            finish_part(1, c, 1)

        loop(DOTS, second)

    def out_arrival(c, q):
        span = PAIR * cols
        place = out.at[0, :, pl.ds(pl.multiple_of(c * side + q * span, span), span)]
        return settle(place, out_r.at[c, q])

    late_factors = factors_of(last)

    def take(q):
        for c in range(2):
            out_arrival(c, q).wait_recv()

            @pl.when(section == 0)
            def _():
                for i in range(PAIR):
                    at = q * PAIR + i
                    where = pl.ds(pl.multiple_of(c * side + at * cols, cols), cols)
                    acc[...] = late_factors[0:1] * out[0, :, where].astype(f32)
                    for k in range(1, slots + 1):

                        @pl.when(gets_last[k - 1])
                        def _():
                            acc[...] += late_factors[k : k + 1] * history_of(k, c, at)

                    out[0, :, where] = acc[...].astype(bf16)

    loop(CHUNKS // PAIR, take)

    settle(chip_rows.at[pl.ds(0, rows)], sib_s).wait_send()

    @pl.when(hi == 1)
    def _():
        settle(peer_rows.at[0], gx_s).wait_send()

    settle(peer_rows.at[0, pl.ds(0, rows - unit)], fw_s).wait_send()

    @pl.when((hi == 0) | (lo == 1))
    def _():
        settle(peer_rows.at[0, pl.ds(0, unit)], fw_s).wait_send()

    @pl.when((hi == 1) & (lo == 1))
    def _():
        settle(peer_rows.at[0, pl.ds(0, unit)], fw_s).wait_send()

    settle(w_out.at[lo], wr_s).wait_send()
    residual_copy().wait_send()
    settle(heads.at[:, lo], hd_s).wait_send()
    for k in range(1, slots + 1):

        @pl.when(gives[k - 1] | gives_last[k - 1])
        def _():
            settle(hist_in.at[k - 1], hist_s.at[k - 1]).wait_send()

    settle(give, xs_s).wait_send()
    settle(mixed, out_s).wait_send()


def solution(mesh):
    sections, tensor = mesh.shape["section"], mesh.shape["tensor"]
    assert tensor == 4

    def on_device(x, history, wq, wk, wv, wo, mix_weights):
        rows, width = x.shape[1:]
        slots = history.shape[1]
        q_width, kv_width = wq.shape[2], wk.shape[2]
        seq = rows * tensor
        tile = 2 * kv_width
        q_tiles = q_width // tile
        side = width // 2
        wide, cols = side // DOTS, side // CHUNKS
        bf16, f32 = jnp.bfloat16, jnp.float32
        dma = pltpu.SemaphoreType.DMA
        hbm = pl.BlockSpec(memory_space=pltpu.HBM)
        factors = mix_weights.T
        return pl.pallas_call(
            functools.partial(tick_kernel, sections),
            out_shape=pltpu.VMEM(x.shape, bf16),
            in_specs=[hbm] * 7,
            out_specs=pl.BlockSpec(memory_space=pltpu.VMEM),
            scratch_shapes=[
                pltpu.VMEM((rows, width), bf16),
                pltpu.VMEM((2, rows, side), bf16),
                pltpu.VMEM((2 * rows, width), bf16),
                pltpu.VMEM((2, rows, width), bf16),
                pltpu.VMEM((q_tiles + 1, width, tile), bf16),
                pltpu.VMEM((2, DOTS, q_width, wide), bf16),
                pltpu.VMEM((2 * q_tiles, seq, kv_width), bf16),
                pltpu.VMEM((kv_width // HEAD_DIM, tensor, 2, rows, kv_width), bf16),
                pltpu.VMEM((kv_width // HEAD_DIM, tensor, 2, rows, 2 * kv_width), bf16),
                pltpu.VMEM((4, 2, rows, q_width), bf16),
                pltpu.VMEM((2, CHUNKS, rows, cols), f32),
                pltpu.VMEM((2, CHUNKS, rows, cols), bf16),
                pltpu.VMEM((2, CHUNKS, rows, cols), bf16),
                pltpu.VMEM((2, CHUNKS, rows, cols), bf16),
                pltpu.VMEM((rows, cols), f32),
                pltpu.VMEM((slots, 2, PASTS, rows, side // PASTS), bf16),
                pltpu.VMEM(factors.shape, factors.dtype),
                dma,
                dma,
                dma((3,)),
                dma,
                dma,
                dma((slots,)),
                dma((slots, 2, PASTS)),
                dma,
                dma,
                dma,
                dma((2, UNITS // 2 + 1)),
                dma,
                dma((2,)),
                dma,
                dma,
                dma,
                dma,
                dma,
                dma((4,)),
                dma,
                dma((2, CHUNKS)),
                dma,
                dma((2, CHUNKS // PAIR)),
                pltpu.SemaphoreType.REGULAR,
                pltpu.SemaphoreType.REGULAR,
                pltpu.SemaphoreType.REGULAR,
            ],
            compiler_params=pltpu.CompilerParams(
                collective_id=0, has_side_effects=True, vmem_limit_bytes=56 * 1024 * 1024
            ),
        )(x, history, wq, wk, wv, wo, factors)

    placed = (
        P("section", "tensor", None),
        P("section", None, "tensor", None),
        P("section", None, "tensor"),
        P("section", None, "tensor"),
        P("section", None, "tensor"),
        P("section", "tensor", None),
        P(),
    )
    return jax.shard_map(
        on_device,
        mesh=mesh,
        in_specs=placed,
        out_specs=P("section", "tensor", None),
        check_vma=False,
    )
```

```python
import functools
import math

import jax
import jax.numpy as jnp
from jax import lax
from jax.experimental import pallas as pl
from jax.experimental.pallas import tpu as pltpu
from jax.sharding import PartitionSpec as P

HEAD_DIM = 64
DILATION_STRIDE = 4
MESH = pl.DeviceIdType.MESH
UNITS = 8
DOTS = 4
CHUNKS = 16
PASTS = 4
PAIR = 2
RELAYS = 1


def start(copy):
    copy.start()
    return copy


def tick_kernel(
    sections,
    x_hbm,
    hist_hbm,
    wq_hbm,
    wk_hbm,
    wv_hbm,
    wo_hbm,
    mix_hbm,
    out,
    x_own,
    x_res,
    chip_rows,
    peer_rows,
    w_all,
    w_out,
    q_all,
    k_pad,
    v_pad,
    heads,
    own_part,
    give,
    x_in,
    mixed,
    acc,
    hist_in,
    mix_v,
    w_sem,
    wo_sem,
    x_sem,
    res_sem,
    mix_sem,
    hist_s,
    hist_r,
    sib_s,
    sib_r,
    gx_s,
    gx_r,
    fw_s,
    fw_r,
    wr_s,
    wr_r,
    xr_s,
    xr_r,
    hd_s,
    hd_r,
    xs_s,
    xs_r,
    out_s,
    out_r,
    relay,
    relay_s,
    relay_r,
    near_sem,
    far_sem,
    clear_sem,
):
    section = lax.axis_index("section")
    me = lax.axis_index("tensor")
    hi, lo = me // 2, me % 2
    sibling = hi * 2 + (1 - lo)
    peer = (1 - hi) * 2 + lo
    rows, width = x_own.shape
    slots = hist_in.shape[0]
    unit = rows // UNITS
    side = width // 2
    wide = side // DOTS
    cols = side // CHUNKS
    per_dot = CHUNKS // DOTS
    past = side // PASTS
    per_past = CHUNKS // PASTS
    q_tiles = w_all.shape[0] - 1
    tile = w_all.shape[2]
    half = tile // 2
    last = sections - 1
    nxt = lax.rem(section + 1, sections)
    prv = lax.rem(section + sections - 1, sections)
    f32, bf16 = jnp.float32, jnp.bfloat16

    middle = (section > 0) & (section < last)
    gets = [middle & (section >= DILATION_STRIDE * k) for k in range(1, slots + 1)]
    gets_last = [(section == 0) & (last >= DILATION_STRIDE * k) for k in range(1, slots + 1)]
    gives = [section + DILATION_STRIDE * k < last for k in range(1, slots + 1)]
    gives_last = [section + DILATION_STRIDE * k == last for k in range(1, slots + 1)]

    def load_unit(i):
        if i < 2:
            at = pl.ds(pl.multiple_of(order[i] * unit, unit), unit)
        else:
            at = pl.ds(2 * unit, rows - 2 * unit)
        return pltpu.make_async_copy(x_hbm.at[0, at], x_own.at[at], x_sem.at[i])

    order = [lo, 1 - lo] + list(range(2, UNITS))
    for i in range(3):
        load_unit(i).start()
    barrier = pltpu.get_barrier_semaphore()

    def greet(s, t):
        pl.semaphore_signal(
            barrier, inc=1, device_id={"section": s, "tensor": t}, device_id_type=MESH
        )

    host = hi == lo
    keeper = hi * 2 + (1 - hi)

    @pl.when(jnp.logical_not(host))
    def _():
        greet(section, sibling)
        greet(section, peer)

    greet(prv, keeper)
    expected = jnp.int32(2)
    for k in range(1, slots + 1):
        step = DILATION_STRIDE * k

        @pl.when(gets[k - 1])
        def _():
            greet(section - step, keeper)

        @pl.when(gets_last[k - 1])
        def _():
            greet(last - step, keeper)

        expected = expected + 2 * (gives[k - 1] | gives_last[k - 1]).astype(jnp.int32)

    vias = [max(last - 2 - r, 0) for r in range(RELAYS)]
    sends_relay = (section == last) & (lo == 1)
    does_relay = [(section == via) & (lo == 1) for via in vias]
    expected = expected + RELAYS * (section == last).astype(jnp.int32)
    for via, does in zip(vias, does_relay):

        @pl.when(does)
        def _():
            greet(last, (1 - hi) * 2 + hi)

        @pl.when(sends_relay)
        def _():
            greet(via, keeper)

        expected = expected + (section == via).astype(jnp.int32)

    loads = [
        pltpu.make_async_copy(
            wk_hbm.at[0], w_all.at[q_tiles, :, pl.ds(0, half)], w_sem
        ),
        pltpu.make_async_copy(
            wv_hbm.at[0], w_all.at[q_tiles, :, pl.ds(half, half)], w_sem
        ),
    ]
    for j in range(q_tiles):
        loads.append(
            pltpu.make_async_copy(
                wq_hbm.at[0, :, pl.ds(j * tile, tile)], w_all.at[j], w_sem
            )
        )
    for copy in loads:
        copy.start()
    load_mix = start(pltpu.make_async_copy(mix_hbm, mix_v, mix_sem))
    mine = pl.multiple_of(lo * rows, rows)
    my_side = pl.multiple_of(lo * side, side)
    other_side = pl.multiple_of((1 - lo) * side, side)

    def norm_unit(u):
        def norm_rows(i, carry):
            at = pl.multiple_of(u * unit + i * 16, 16)
            values = x_own[pl.ds(at, 16), :].astype(f32)
            inv = lax.rsqrt(jnp.mean(values * values, axis=-1, keepdims=True) + 1e-05)
            chip_rows[pl.ds(pl.multiple_of(mine + at, 16), 16), :] = (values * inv).astype(bf16)
            return carry

        lax.fori_loop(0, unit // 16, norm_rows, 0)

    def remote(src, dst, send, recv, s, t):
        return pltpu.make_async_remote_copy(
            src_ref=src,
            dst_ref=dst,
            send_sem=send,
            recv_sem=recv,
            device_id={"section": s, "tensor": t},
            device_id_type=MESH,
        )

    def settle(place, sem):
        return remote(place, place, sem, sem, section, sibling)

    def sibling_copy(u):
        place = chip_rows.at[pl.ds(pl.multiple_of(mine + u * unit, unit), unit)]
        return remote(place, place, sib_s, sib_r, section, sibling)

    share = UNITS // 2

    def unit_of(i):
        return UNITS - 2 if i == share else 2 * i + lo

    def gather_copy(j, i):
        at = unit_of(i) * unit
        return remote(
            chip_rows.at[pl.ds(pl.multiple_of(j * rows + at, unit), unit)],
            peer_rows.at[j, pl.ds(pl.multiple_of(at, unit), unit)],
            gx_s,
            gx_r.at[j, i],
            section,
            peer,
        )

    def forward_copy(j, i):
        place = peer_rows.at[j, pl.ds(pl.multiple_of(unit_of(i) * unit, unit), unit)]
        return remote(place, place, fw_s, fw_r.at[j], section, sibling)

    def hist_copy(k, c, q, to_last):
        src = hist_hbm.at[0, k - 1, :, pl.ds(pl.multiple_of(c * side + q * past, past), past)]
        slot = c if to_last else lo
        if to_last:
            s, t = 0, me
        else:
            s, t = section + DILATION_STRIDE * k, hi * 2 + c
        return remote(
            src,
            hist_in.at[k - 1, slot, q],
            hist_s.at[k - 1],
            hist_r.at[k - 1, slot, q],
            s,
            t,
        )

    def send_history():
        for k in range(1, slots + 1):
            for to_last, sends in ((False, gives[k - 1]), (True, gives_last[k - 1])):

                @pl.when(sends)
                def _():
                    def each(q, carry):
                        for c in range(2):
                            hist_copy(k, c, q, to_last).start()
                        return carry

                    lax.fori_loop(0, PASTS, each, 0)

    late = (lo == 1) & (section % 2 == 0)
    latest = late & (section % DILATION_STRIDE == 0)

    def tell(sem, t):
        pl.semaphore_signal(
            sem, inc=1, device_id={"section": section, "tensor": t}, device_id_type=MESH
        )

    load_unit(0).wait()
    norm_unit(order[0])

    @pl.when(host)
    def _():
        pl.semaphore_wait(barrier, 2)
        gather_copy(lo, 0).start()
        tell(near_sem, sibling)
        tell(near_sem, peer)
        sibling_copy(order[0]).start()

    load_unit(1).wait()
    norm_unit(order[1])

    @pl.when(jnp.logical_not(host))
    def _():
        pl.semaphore_wait(near_sem, 2)
        gather_copy(lo, 0).start()
        sibling_copy(order[0]).start()

    sibling_copy(order[1]).start()
    load_unit(2).wait()
    for i in range(2, UNITS):
        norm_unit(order[i])
        sibling_copy(order[i]).start()
        if i % 2 == 0:

            @pl.when(lo == 0)
            def _():
                gather_copy(0, i // 2).start()

    settle(chip_rows.at[pl.ds(0, rows)], sib_r).wait_recv()

    @pl.when(lo == 0)
    def _():
        for i in range(share - 1):
            gather_copy(1, i).start()

        @pl.when(hi == 1)
        def _():
            gather_copy(1, share - 1).start()

    @pl.when(lo == 1)
    def _():
        for i in range(share):
            gather_copy(0, i).start()
        for i in range(1, share - RELAYS):
            gather_copy(1, i).start()

        @pl.when(hi == 0)
        def _():
            gather_copy(1, share).start()

        @pl.when(section < last)
        def _():
            for i in range(share - RELAYS, share):
                gather_copy(1, i).start()

    @pl.when(jnp.logical_not(host))
    def _():
        pl.semaphore_wait(barrier, expected)
        tell(far_sem, sibling)

    @pl.when(host)
    def _():
        pl.semaphore_wait(far_sem, 1)

    def relay_in(r):
        src = chip_rows.at[pl.ds(2 * rows - (2 * r + 1) * unit, unit)]
        return remote(src, relay.at[r], gx_s, relay_r.at[r], vias[r], peer)

    def relay_out(r):
        place = peer_rows.at[1, pl.ds(rows - (2 * r + 1) * unit, unit)]
        return remote(
            relay.at[r], place, relay_s.at[r], gx_r.at[1, share - 1 - r], last, me
        )

    @pl.when(sends_relay)
    def _():
        for r in range(RELAYS):
            relay_in(r).start()

    @pl.when(jnp.logical_not(late))
    def _():
        send_history()

    def weight_copy(c):
        return remote(
            wo_hbm.at[0, :, pl.ds(pl.multiple_of(other_side + c * wide, wide), wide)],
            w_out.at[lo, c],
            wr_s,
            wr_r,
            section,
            sibling,
        )

    def residual_copy():
        return remote(
            x_own.at[:, pl.ds(other_side, side)], x_res.at[lo], xr_s, xr_r, section, sibling
        )

    for c in range(DOTS):
        pltpu.make_async_copy(
            wo_hbm.at[0, :, pl.ds(pl.multiple_of(my_side + c * wide, wide), wide)],
            w_out.at[lo, c],
            wo_sem,
        ).start()
        weight_copy(c).start()
    load_res = start(
        pltpu.make_async_copy(x_hbm.at[0, :, pl.ds(my_side, side)], x_res.at[lo], res_sem)
    )
    residual_copy().start()

    scale = 1.0 / math.sqrt(HEAD_DIM)

    def project_query(rows_ref, target):
        size = rows_ref.shape[0]
        where = pl.ds(pl.multiple_of(target, size), size)

        def q_tile(j, carry):
            got = jnp.dot(rows_ref[...], w_all[j], preferred_element_type=f32)
            got = got.astype(bf16) * bf16(scale)
            q_all[2 * j, where, :] = got[:, :half]
            q_all[2 * j + 1, where, :] = got[:, half:]
            return carry

        lax.fori_loop(0, q_tiles, q_tile, 0)

    def project_key_value(rows_ref, first):
        size = rows_ref.shape[0]
        got = jnp.dot(rows_ref[...], w_all[q_tiles], preferred_element_type=f32)
        got = got.astype(bf16).astype(f32)
        for part, padded in ((got[:, :half], k_pad), (got[:, half:], v_pad)):
            lane = lax.broadcasted_iota(jnp.int32, part.shape, 1)
            turned = pltpu.roll(part, HEAD_DIM, 1)
            low = lane < HEAD_DIM
            zero = jnp.zeros_like(part)
            forms = (
                jnp.where(low, part, zero),
                jnp.where(low, zero, turned),
                jnp.where(low, turned, zero),
                jnp.where(low, zero, part),
            )
            for f, form in enumerate(forms):
                for i in range(size // rows):
                    some = form[i * rows : (i + 1) * rows].astype(bf16)
                    padded[f // 2, first + i, f % 2, :, :half] = some

    def fill_ones():
        low = lax.broadcasted_iota(jnp.int32, (rows, half), 1) < HEAD_DIM
        for which in range(2):
            ones = jnp.where(low == (which == 0), 1.0, 0.0).astype(bf16)
            for kv in range(v_pad.shape[0]):
                for i in range(v_pad.shape[1]):
                    v_pad[kv, i, which, :, half:] = ones

    pairs = q_all.shape[0]
    pairs_per_kv = pairs // (half // HEAD_DIM)

    def heads_copy(t, kv):
        span = pairs_per_kv * half
        place = heads.at[t, lo, :, pl.ds(pl.multiple_of(kv * span, span), span)]
        return remote(place, place, hd_s, hd_r.at[t], section, sibling)

    def heads_ready(t):
        settle(heads.at[t, 1 - lo], hd_r.at[t]).wait_recv()

    def attend(t, after=None):
        first, blocks = t * rows, t + 1
        seen = lax.broadcasted_iota(jnp.int32, (rows, rows), 0) >= lax.broadcasted_iota(
            jnp.int32, (rows, rows), 1
        )

        def exponents(scores, which):
            mine = [
                scores[:, (2 * i + which) * rows : (2 * i + which + 1) * rows]
                for i in range(blocks)
            ]
            mine[t] = jnp.where(seen, mine[t], -1e30)
            top = jnp.max(functools.reduce(jnp.maximum, mine), axis=-1, keepdims=True)
            return [jnp.exp(part - top).astype(bf16) for part in mine]

        def group(kv, carry):
            keys = k_pad[kv, :blocks].reshape(2 * blocks * rows, half)
            values = v_pad[kv, :blocks].reshape(2 * blocks * rows, 2 * half)
            scores = [
                lax.dot_general(
                    q_all[kv * pairs_per_kv + i, first : first + rows, :],
                    keys,
                    (((1,), (1,)), ((), ())),
                    preferred_element_type=f32,
                )
                for i in range(pairs_per_kv)
            ]
            probs = []
            for got in scores:
                even, odd = exponents(got, 0), exponents(got, 1)
                both = [part for pair in zip(even, odd) for part in pair]
                probs.append(jnp.concatenate(both, axis=1))
            for i, weights in enumerate(probs):
                both = jnp.dot(weights, values, preferred_element_type=f32)
                total = both[:, :half] / both[:, half:]
                at = pl.multiple_of((kv * pairs_per_kv + i) * half, half)
                heads[t, lo, :, pl.ds(at, half)] = total.astype(bf16)
            heads_copy(t, kv).start()
            if after is not None:
                after(kv)
            return carry

        lax.fori_loop(0, pairs // pairs_per_kv, group, 0)

    def out_dot(t, c):
        got = jnp.dot(heads[t, 0], w_out[0, c], preferred_element_type=f32)
        return got + jnp.dot(heads[t, 1], w_out[1, c], preferred_element_type=f32)

    def cross_copy(j, q):
        return remote(give.at[j, q], x_in.at[j, q], xs_s, xs_r.at[j, q], section, peer)

    def peer_output(t, j, c, send=True):
        got = out_dot(t, c).astype(bf16)
        for i in range(per_dot):
            give[j, c * per_dot + i] = got[:, i * cols : (i + 1) * cols]
            if send:
                cross_copy(j, c * per_dot + i).start()

    def own_output(t, j, c):
        got = out_dot(t, c)
        for i in range(per_dot):
            own_part[j, c * per_dot + i] = got[:, i * cols : (i + 1) * cols]

    def own_half(t, j, c, core):
        got = jnp.dot(heads[t, core], w_out[core, c], preferred_element_type=f32)
        for i in range(per_dot):
            part = got[:, i * cols : (i + 1) * cols]
            if core is lo:
                own_part[j, c * per_dot + i] = part
            else:
                own_part[j, c * per_dot + i] += part

    def loop(count, body):
        def step(i, carry):
            body(i)
            return carry

        lax.fori_loop(0, count, step, 0)

    def out_copy(j, q):
        return remote(
            mixed.at[j, q],
            out.at[0, :, pl.ds(pl.multiple_of(my_side + q * cols, cols), cols)],
            out_s,
            out_r.at[lo, q // PAIR],
            nxt,
            hi * 2 + j,
        )

    def hist_arrival(k, i, q):
        place = hist_in.at[k - 1, i, q]
        return remote(
            place, place, hist_s.at[k - 1], hist_r.at[k - 1, i, q], section, sibling
        )

    def history_of(k, i, q):
        @pl.when(q % per_past == 0)
        def _():
            hist_arrival(k, i, q // per_past).wait_recv()

        where = pl.ds(pl.multiple_of((q % per_past) * cols, cols), cols)
        return hist_in[k - 1, i, q // per_past, :, where].astype(f32)

    load_mix.wait()
    position = lax.broadcasted_iota(jnp.int32, mix_v.shape, 1)

    def factors_of(s):
        return jnp.sum(jnp.where(position == s, mix_v[...], 0.0), axis=1, keepdims=True)

    factors = factors_of(section)
    plain = jnp.where(section == last, jnp.ones_like(factors[0:1]), factors[0:1])

    def finish(j, q):
        cross_copy(j, q).wait_recv()
        total = own_part[j, q] + x_in[j, q].astype(f32)
        given = x_res[j, :, pl.ds(pl.multiple_of(q * cols, cols), cols)].astype(f32)
        block = (given + total).astype(bf16)
        acc[...] = plain * block.astype(f32)
        for k in range(1, slots + 1):

            @pl.when(gets[k - 1])
            def _():
                acc[...] += factors[k : k + 1] * history_of(k, j, q)

        mixed[j, q] = acc[...].astype(bf16)
        out_copy(j, q).start()

    def receive_block(j, then=None):
        def pass_on(i):
            gather_copy(j, i).wait_recv()
            forward_copy(j, i).start()

        def passed(count):
            settle(peer_rows.at[j, pl.ds(0, count * unit)], fw_r.at[j]).wait_recv()

        if j == 0:
            for i in range(share):
                pass_on(i)
            passed(share)
            return
        for i in range(share - 1):
            pass_on(i)

        @pl.when((hi == 1) & (lo == 1))
        def _():
            pass_on(share)

        @pl.when((hi == 0) | (lo == 1))
        def _():
            pass_on(share - 1)

        then()

        @pl.when(hi == 0)
        def _():
            passed(share)

        @pl.when((hi == 1) & (lo == 0))
        def _():
            passed(share + 1)

        @pl.when((hi == 1) & (lo == 1))
        def _():
            passed(share - 1)

    fill_ones()
    pltpu.make_async_copy(w_all, w_all, w_sem).wait()
    project_key_value(chip_rows, hi * 2)
    project_query(chip_rows, hi * 2 * rows)

    def out_weights_ready():
        pltpu.make_async_copy(w_out.at[lo], w_out.at[lo], wo_sem).wait()
        settle(w_out.at[1 - lo], wr_r).wait_recv()
        load_res.wait()
        residual_copy().wait_recv()

    def peer_block(j):
        target = ((1 - hi) * 2 + j) * rows
        return peer_rows.at[j], target

    @pl.when(hi == 0)
    def _():
        attend(0)
        attend(1)

    out_weights_ready()

    @pl.when(hi == 0)
    def _():
        for j in range(2):
            heads_ready(j)
            loop(DOTS, lambda c: own_output(j, j, c))

    for r in range(RELAYS):

        @pl.when(does_relay[r])
        def _():
            relay_in(r).wait_recv()
            relay_out(r).start()

    receive_block(0)
    project_key_value(peer_rows.at[0], (1 - hi) * 2)
    project_query(*peer_block(0))

    @pl.when(hi == 0)
    def _():
        attend(2)

        @pl.when(jnp.logical_not(host))
        def _():
            settle(peer_rows.at[0], gx_s).wait_send()
            settle(peer_rows.at[0, pl.ds(0, unit)], gx_s).wait_send()
            tell(clear_sem, sibling)
            heads_ready(2)
            loop(DOTS, lambda c: peer_output(2, 0, c))

        @pl.when(host)
        def _():
            heads_ready(2)
            loop(DOTS, lambda c: peer_output(2, 0, c, False))
            settle(peer_rows.at[0, pl.ds(0, rows - unit)], gx_s).wait_send()
            pl.semaphore_wait(clear_sem, 1)
            loop(CHUNKS, lambda q: cross_copy(0, q).start())


    @pl.when(hi == 1)
    def _():
        attend(0)
        heads_ready(0)
        loop(DOTS, lambda c: peer_output(0, 0, c))

    @pl.when(late & jnp.logical_not(latest))
    def _():
        send_history()

    def finish_part(j, c, parts=2):
        count = CHUNKS // (parts * DOTS)
        loop(count, lambda i: finish(j, c * count + i))

    def first_part():
        @pl.when(hi == 0)
        def _():
            finish_part(0, 0)

    receive_block(1, first_part)
    project_key_value(peer_rows.at[1], (1 - hi) * 2 + 1)

    @pl.when(hi == 0)
    def _():
        project_query(*peer_block(1))
        finish_part(0, 1)
        attend(3, lambda kv: finish_part(0, 2 + kv))

        @pl.when(latest)
        def _():
            send_history()

        finish_part(0, 4)
        heads_ready(3)

        def step(c):
            peer_output(3, 1, c)

            @pl.when(c > 0)
            def _():
                finish_part(0, 4 + c)

        loop(DOTS, step)
        loop(CHUNKS, lambda q: finish(1, q))

    @pl.when(hi == 1)
    def _():
        attend(2)
        loop(DOTS, lambda c: own_half(2, 0, c, lo))
        heads_ready(2)
        own_half(2, 0, 0, 1 - lo)
        finish_part(0, 0, 1)
        project_query(*peer_block(1))
        attend(1)

        @pl.when(latest)
        def _():
            send_history()

        own_half(2, 0, 1, 1 - lo)
        finish_part(0, 1, 1)
        heads_ready(1)

        def first(c):
            peer_output(1, 1, c)

            @pl.when(c < DOTS - 2)
            def _():
                own_half(2, 0, 2 + c, 1 - lo)
                finish_part(0, 2 + c, 1)

        loop(DOTS, first)
        attend(3)
        heads_ready(3)

        def second(c):
            own_output(3, 1, c)
            finish_part(1, c, 1)

        loop(DOTS, second)

    def out_arrival(c, q):
        span = PAIR * cols
        place = out.at[0, :, pl.ds(pl.multiple_of(c * side + q * span, span), span)]
        return settle(place, out_r.at[c, q])

    late_factors = factors_of(last)

    def take(q):
        for c in range(2):
            out_arrival(c, q).wait_recv()

            @pl.when(section == 0)
            def _():
                for i in range(PAIR):
                    at = q * PAIR + i
                    where = pl.ds(pl.multiple_of(c * side + at * cols, cols), cols)
                    acc[...] = late_factors[0:1] * out[0, :, where].astype(f32)
                    for k in range(1, slots + 1):

                        @pl.when(gets_last[k - 1])
                        def _():
                            acc[...] += late_factors[k : k + 1] * history_of(k, c, at)

                    out[0, :, where] = acc[...].astype(bf16)

    loop(CHUNKS // PAIR, take)

    settle(chip_rows.at[pl.ds(0, rows)], sib_s).wait_send()

    @pl.when(hi == 1)
    def _():
        settle(peer_rows.at[0], gx_s).wait_send()

    settle(peer_rows.at[0, pl.ds(0, rows - unit)], fw_s).wait_send()

    @pl.when((hi == 0) | (lo == 1))
    def _():
        settle(peer_rows.at[0, pl.ds(0, unit)], fw_s).wait_send()

    @pl.when((hi == 1) & (lo == 1))
    def _():
        settle(peer_rows.at[0, pl.ds(0, unit)], fw_s).wait_send()

    settle(w_out.at[lo], wr_s).wait_send()
    residual_copy().wait_send()
    settle(heads.at[:, lo], hd_s).wait_send()
    for k in range(1, slots + 1):

        @pl.when(gives[k - 1] | gives_last[k - 1])
        def _():
            settle(hist_in.at[k - 1], hist_s.at[k - 1]).wait_send()

    settle(give, xs_s).wait_send()
    settle(mixed, out_s).wait_send()

    for r in range(RELAYS):

        @pl.when(does_relay[r])
        def _():
            relay_out(r).wait_send()


def solution(mesh):
    sections, tensor = mesh.shape["section"], mesh.shape["tensor"]
    assert tensor == 4

    def on_device(x, history, wq, wk, wv, wo, mix_weights):
        rows, width = x.shape[1:]
        slots = history.shape[1]
        q_width, kv_width = wq.shape[2], wk.shape[2]
        seq = rows * tensor
        tile = 2 * kv_width
        q_tiles = q_width // tile
        side = width // 2
        wide, cols = side // DOTS, side // CHUNKS
        bf16, f32 = jnp.bfloat16, jnp.float32
        dma = pltpu.SemaphoreType.DMA
        hbm = pl.BlockSpec(memory_space=pltpu.HBM)
        factors = mix_weights.T
        return pl.pallas_call(
            functools.partial(tick_kernel, sections),
            out_shape=pltpu.VMEM(x.shape, bf16),
            in_specs=[hbm] * 7,
            out_specs=pl.BlockSpec(memory_space=pltpu.VMEM),
            scratch_shapes=[
                pltpu.VMEM((rows, width), bf16),
                pltpu.VMEM((2, rows, side), bf16),
                pltpu.VMEM((2 * rows, width), bf16),
                pltpu.VMEM((2, rows, width), bf16),
                pltpu.VMEM((q_tiles + 1, width, tile), bf16),
                pltpu.VMEM((2, DOTS, q_width, wide), bf16),
                pltpu.VMEM((2 * q_tiles, seq, kv_width), bf16),
                pltpu.VMEM((kv_width // HEAD_DIM, tensor, 2, rows, kv_width), bf16),
                pltpu.VMEM((kv_width // HEAD_DIM, tensor, 2, rows, 2 * kv_width), bf16),
                pltpu.VMEM((4, 2, rows, q_width), bf16),
                pltpu.VMEM((2, CHUNKS, rows, cols), f32),
                pltpu.VMEM((2, CHUNKS, rows, cols), bf16),
                pltpu.VMEM((2, CHUNKS, rows, cols), bf16),
                pltpu.VMEM((2, CHUNKS, rows, cols), bf16),
                pltpu.VMEM((rows, cols), f32),
                pltpu.VMEM((slots, 2, PASTS, rows, side // PASTS), bf16),
                pltpu.VMEM(factors.shape, factors.dtype),
                dma,
                dma,
                dma((3,)),
                dma,
                dma,
                dma((slots,)),
                dma((slots, 2, PASTS)),
                dma,
                dma,
                dma,
                dma((2, UNITS // 2 + 1)),
                dma,
                dma((2,)),
                dma,
                dma,
                dma,
                dma,
                dma,
                dma((4,)),
                dma,
                dma((2, CHUNKS)),
                dma,
                dma((2, CHUNKS // PAIR)),
                pltpu.VMEM((RELAYS, rows // UNITS, width), bf16),
                dma((RELAYS,)),
                dma((RELAYS,)),
                pltpu.SemaphoreType.REGULAR,
                pltpu.SemaphoreType.REGULAR,
                pltpu.SemaphoreType.REGULAR,
            ],
            compiler_params=pltpu.CompilerParams(
                collective_id=0, has_side_effects=True, vmem_limit_bytes=56 * 1024 * 1024
            ),
        )(x, history, wq, wk, wv, wo, factors)

    placed = (
        P("section", "tensor", None),
        P("section", None, "tensor", None),
        P("section", None, "tensor"),
        P("section", None, "tensor"),
        P("section", None, "tensor"),
        P("section", "tensor", None),
        P(),
    )
    return jax.shard_map(
        on_device,
        mesh=mesh,
        in_specs=placed,
        out_specs=P("section", "tensor", None),
        check_vma=False,
    )
```

```python
import functools
import math

import jax
import jax.numpy as jnp
from jax import lax
from jax.experimental import pallas as pl
from jax.experimental.pallas import tpu as pltpu
from jax.sharding import PartitionSpec as P

HEAD_DIM = 64
DILATION_STRIDE = 4
MESH = pl.DeviceIdType.MESH
UNITS = 8
DOTS = 4
CHUNKS = 16
PASTS = 4
PAIR = 2
RELAYS = 1


def start(copy):
    copy.start()
    return copy


def tick_kernel(
    sections,
    x_hbm,
    hist_hbm,
    wq_hbm,
    wk_hbm,
    wv_hbm,
    wo_hbm,
    mix_hbm,
    out,
    x_own,
    x_res,
    chip_rows,
    peer_rows,
    w_all,
    w_out,
    q_all,
    k_pad,
    v_pad,
    heads,
    own_part,
    give,
    x_in,
    mixed,
    acc,
    hist_in,
    mix_v,
    w_sem,
    wo_sem,
    x_sem,
    res_sem,
    mix_sem,
    hist_s,
    hist_r,
    sib_s,
    sib_r,
    gx_s,
    gx_r,
    fw_s,
    fw_r,
    wr_s,
    wr_r,
    xr_s,
    xr_r,
    hd_s,
    hd_r,
    xs_s,
    xs_r,
    out_s,
    out_r,
    relay,
    relay_s,
    relay_r,
    near_sem,
    far_sem,
    clear_sem,
):
    section = lax.axis_index("section")
    me = lax.axis_index("tensor")
    hi, lo = me // 2, me % 2
    sibling = hi * 2 + (1 - lo)
    peer = (1 - hi) * 2 + lo
    rows, width = x_own.shape
    slots = hist_in.shape[0]
    unit = rows // UNITS
    side = width // 2
    wide = side // DOTS
    cols = side // CHUNKS
    per_dot = CHUNKS // DOTS
    past = side // PASTS
    per_past = CHUNKS // PASTS
    q_tiles = w_all.shape[0] - 1
    tile = w_all.shape[2]
    half = tile // 2
    last = sections - 1
    nxt = lax.rem(section + 1, sections)
    prv = lax.rem(section + sections - 1, sections)
    f32, bf16 = jnp.float32, jnp.bfloat16

    middle = (section > 0) & (section < last)
    gets = [middle & (section >= DILATION_STRIDE * k) for k in range(1, slots + 1)]
    gets_last = [(section == 0) & (last >= DILATION_STRIDE * k) for k in range(1, slots + 1)]
    gives = [section + DILATION_STRIDE * k < last for k in range(1, slots + 1)]
    gives_last = [section + DILATION_STRIDE * k == last for k in range(1, slots + 1)]

    def load_unit(i):
        if i < 2:
            at = pl.ds(pl.multiple_of(order[i] * unit, unit), unit)
        else:
            at = pl.ds(2 * unit, rows - 2 * unit)
        return pltpu.make_async_copy(x_hbm.at[0, at], x_own.at[at], x_sem.at[i])

    order = [lo, 1 - lo] + list(range(2, UNITS))
    for i in range(3):
        load_unit(i).start()
    barrier = pltpu.get_barrier_semaphore()

    def greet(s, t):
        pl.semaphore_signal(
            barrier, inc=1, device_id={"section": s, "tensor": t}, device_id_type=MESH
        )

    host = hi == lo
    keeper = hi * 2 + (1 - hi)

    @pl.when(jnp.logical_not(host))
    def _():
        greet(section, sibling)
        greet(section, peer)

    greet(prv, keeper)
    expected = jnp.int32(2)
    for k in range(1, slots + 1):
        step = DILATION_STRIDE * k

        @pl.when(gets[k - 1])
        def _():
            greet(section - step, keeper)

        @pl.when(gets_last[k - 1])
        def _():
            greet(last - step, keeper)

        expected = expected + 2 * (gives[k - 1] | gives_last[k - 1]).astype(jnp.int32)

    vias = [max(last - 2 - r, 0) for r in range(RELAYS)]
    sends_relay = (section == last) & (lo == 1)
    does_relay = [(section == via) & (lo == 1) for via in vias]
    expected = expected + RELAYS * (section == last).astype(jnp.int32)
    for via, does in zip(vias, does_relay):

        @pl.when(does)
        def _():
            greet(last, (1 - hi) * 2 + hi)

        @pl.when(sends_relay)
        def _():
            greet(via, keeper)

        expected = expected + (section == via).astype(jnp.int32)

    loads = [
        pltpu.make_async_copy(
            wk_hbm.at[0], w_all.at[q_tiles, :, pl.ds(0, half)], w_sem
        ),
        pltpu.make_async_copy(
            wv_hbm.at[0], w_all.at[q_tiles, :, pl.ds(half, half)], w_sem
        ),
    ]
    for j in range(q_tiles):
        loads.append(
            pltpu.make_async_copy(
                wq_hbm.at[0, :, pl.ds(j * tile, tile)], w_all.at[j], w_sem
            )
        )
    for copy in loads:
        copy.start()
    load_mix = start(pltpu.make_async_copy(mix_hbm, mix_v, mix_sem))
    mine = pl.multiple_of(lo * rows, rows)
    my_side = pl.multiple_of(lo * side, side)
    other_side = pl.multiple_of((1 - lo) * side, side)

    def norm_unit(u):
        def norm_rows(i, carry):
            at = pl.multiple_of(u * unit + i * 16, 16)
            values = x_own[pl.ds(at, 16), :].astype(f32)
            inv = lax.rsqrt(jnp.mean(values * values, axis=-1, keepdims=True) + 1e-05)
            chip_rows[pl.ds(pl.multiple_of(mine + at, 16), 16), :] = (values * inv).astype(bf16)
            return carry

        lax.fori_loop(0, unit // 16, norm_rows, 0)

    def remote(src, dst, send, recv, s, t):
        return pltpu.make_async_remote_copy(
            src_ref=src,
            dst_ref=dst,
            send_sem=send,
            recv_sem=recv,
            device_id={"section": s, "tensor": t},
            device_id_type=MESH,
        )

    def settle(place, sem):
        return remote(place, place, sem, sem, section, sibling)

    def sibling_copy(u):
        place = chip_rows.at[pl.ds(pl.multiple_of(mine + u * unit, unit), unit)]
        return remote(place, place, sib_s, sib_r, section, sibling)

    share = UNITS // 2

    def unit_of(i):
        return UNITS - 2 if i == share else 2 * i + lo

    def gather_copy(j, i):
        at = unit_of(i) * unit
        return remote(
            chip_rows.at[pl.ds(pl.multiple_of(j * rows + at, unit), unit)],
            peer_rows.at[j, pl.ds(pl.multiple_of(at, unit), unit)],
            gx_s,
            gx_r.at[j, i],
            section,
            peer,
        )

    def forward_copy(j, i):
        place = peer_rows.at[j, pl.ds(pl.multiple_of(unit_of(i) * unit, unit), unit)]
        return remote(place, place, fw_s, fw_r.at[j], section, sibling)

    def hist_copy(k, c, q, to_last):
        src = hist_hbm.at[0, k - 1, :, pl.ds(pl.multiple_of(c * side + q * past, past), past)]
        slot = c if to_last else lo
        if to_last:
            s, t = 0, me
        else:
            s, t = section + DILATION_STRIDE * k, hi * 2 + c
        return remote(
            src,
            hist_in.at[k - 1, slot, q],
            hist_s.at[k - 1],
            hist_r.at[k - 1, slot, q],
            s,
            t,
        )

    def send_history():
        for k in range(1, slots + 1):
            for to_last, sends in ((False, gives[k - 1]), (True, gives_last[k - 1])):

                @pl.when(sends)
                def _():
                    def each(q, carry):
                        for c in range(2):
                            hist_copy(k, c, q, to_last).start()
                        return carry

                    lax.fori_loop(0, PASTS, each, 0)

    late = (lo == 1) & (section % 2 == 0)
    latest = late & (section % DILATION_STRIDE == 0)

    def tell(sem, t):
        pl.semaphore_signal(
            sem, inc=1, device_id={"section": section, "tensor": t}, device_id_type=MESH
        )

    load_unit(0).wait()
    norm_unit(order[0])

    @pl.when(host)
    def _():
        pl.semaphore_wait(barrier, 2)
        gather_copy(lo, 0).start()
        tell(near_sem, sibling)
        tell(near_sem, peer)
        sibling_copy(order[0]).start()

    load_unit(1).wait()
    norm_unit(order[1])

    @pl.when(jnp.logical_not(host))
    def _():
        pl.semaphore_wait(near_sem, 2)
        gather_copy(lo, 0).start()
        sibling_copy(order[0]).start()

    sibling_copy(order[1]).start()
    load_unit(2).wait()
    for i in range(2, UNITS):
        norm_unit(order[i])
        sibling_copy(order[i]).start()
        if i % 2 == 0:

            @pl.when(lo == 0)
            def _():
                gather_copy(0, i // 2).start()

    settle(chip_rows.at[pl.ds(0, rows)], sib_r).wait_recv()

    @pl.when(lo == 0)
    def _():
        for i in range(share - 1):
            gather_copy(1, i).start()

        @pl.when(hi == 1)
        def _():
            gather_copy(1, share - 1).start()

    @pl.when(lo == 1)
    def _():
        for i in range(share):
            gather_copy(0, i).start()
        for i in range(1, share - RELAYS):
            gather_copy(1, i).start()

        @pl.when(hi == 0)
        def _():
            gather_copy(1, share).start()

        @pl.when(section < last)
        def _():
            for i in range(share - RELAYS, share):
                gather_copy(1, i).start()

    @pl.when(jnp.logical_not(host))
    def _():
        pl.semaphore_wait(barrier, expected)
        tell(far_sem, sibling)

    @pl.when(host)
    def _():
        pl.semaphore_wait(far_sem, 1)

    def relay_in(r):
        src = chip_rows.at[pl.ds(2 * rows - (2 * r + 1) * unit, unit)]
        return remote(src, relay.at[r], gx_s, relay_r.at[r], vias[r], peer)

    def relay_out(r):
        place = peer_rows.at[1, pl.ds(rows - (2 * r + 1) * unit, unit)]
        return remote(
            relay.at[r], place, relay_s.at[r], gx_r.at[1, share - 1 - r], last, me
        )

    @pl.when(sends_relay)
    def _():
        for r in range(RELAYS):
            relay_in(r).start()

    @pl.when(jnp.logical_not(late))
    def _():
        send_history()

    def weight_copy(c):
        return remote(
            wo_hbm.at[0, :, pl.ds(pl.multiple_of(other_side + c * wide, wide), wide)],
            w_out.at[lo, c],
            wr_s,
            wr_r,
            section,
            sibling,
        )

    def residual_copy():
        return remote(
            x_own.at[:, pl.ds(other_side, side)], x_res.at[lo], xr_s, xr_r, section, sibling
        )

    for c in range(DOTS):
        pltpu.make_async_copy(
            wo_hbm.at[0, :, pl.ds(pl.multiple_of(my_side + c * wide, wide), wide)],
            w_out.at[lo, c],
            wo_sem,
        ).start()
        weight_copy(c).start()
    load_res = start(
        pltpu.make_async_copy(x_hbm.at[0, :, pl.ds(my_side, side)], x_res.at[lo], res_sem)
    )
    residual_copy().start()

    scale = 1.0 / math.sqrt(HEAD_DIM)

    def project_query(rows_ref, target):
        size = rows_ref.shape[0]
        where = pl.ds(pl.multiple_of(target, size), size)

        def q_tile(j, carry):
            got = jnp.dot(rows_ref[...], w_all[j], preferred_element_type=f32)
            got = got.astype(bf16) * bf16(scale)
            q_all[2 * j, where, :] = got[:, :half]
            q_all[2 * j + 1, where, :] = got[:, half:]
            return carry

        lax.fori_loop(0, q_tiles, q_tile, 0)

    def project_key_value(rows_ref, first):
        size = rows_ref.shape[0]
        got = jnp.dot(rows_ref[...], w_all[q_tiles], preferred_element_type=f32)
        got = got.astype(bf16).astype(f32)
        for part, padded in ((got[:, :half], k_pad), (got[:, half:], v_pad)):
            lane = lax.broadcasted_iota(jnp.int32, part.shape, 1)
            turned = pltpu.roll(part, HEAD_DIM, 1)
            low = lane < HEAD_DIM
            zero = jnp.zeros_like(part)
            forms = (
                jnp.where(low, part, zero),
                jnp.where(low, zero, turned),
                jnp.where(low, turned, zero),
                jnp.where(low, zero, part),
            )
            for f, form in enumerate(forms):
                for i in range(size // rows):
                    some = form[i * rows : (i + 1) * rows].astype(bf16)
                    padded[f // 2, first + i, f % 2, :, :half] = some

    def fill_ones():
        low = lax.broadcasted_iota(jnp.int32, (rows, half), 1) < HEAD_DIM
        for which in range(2):
            ones = jnp.where(low == (which == 0), 1.0, 0.0).astype(bf16)
            for kv in range(v_pad.shape[0]):
                for i in range(v_pad.shape[1]):
                    v_pad[kv, i, which, :, half:] = ones

    pairs = q_all.shape[0]
    pairs_per_kv = pairs // (half // HEAD_DIM)

    def heads_copy(t, kv):
        span = pairs_per_kv * half
        place = heads.at[t, lo, :, pl.ds(pl.multiple_of(kv * span, span), span)]
        return remote(place, place, hd_s, hd_r.at[t], section, sibling)

    def heads_ready(t):
        settle(heads.at[t, 1 - lo], hd_r.at[t]).wait_recv()

    def attend(t, after=None):
        first, blocks = t * rows, t + 1
        seen = lax.broadcasted_iota(jnp.int32, (rows, rows), 0) >= lax.broadcasted_iota(
            jnp.int32, (rows, rows), 1
        )

        def exponents(scores, which):
            mine = [
                scores[:, (2 * i + which) * rows : (2 * i + which + 1) * rows]
                for i in range(blocks)
            ]
            mine[t] = jnp.where(seen, mine[t], -1e30)
            top = jnp.max(functools.reduce(jnp.maximum, mine), axis=-1, keepdims=True)
            return [jnp.exp(part - top).astype(bf16) for part in mine]

        def group(kv, carry):
            keys = k_pad[kv, :blocks].reshape(2 * blocks * rows, half)
            values = v_pad[kv, :blocks].reshape(2 * blocks * rows, 2 * half)
            scores = [
                lax.dot_general(
                    q_all[kv * pairs_per_kv + i, first : first + rows, :],
                    keys,
                    (((1,), (1,)), ((), ())),
                    preferred_element_type=f32,
                )
                for i in range(pairs_per_kv)
            ]
            probs = []
            for got in scores:
                even, odd = exponents(got, 0), exponents(got, 1)
                both = [part for pair in zip(even, odd) for part in pair]
                probs.append(jnp.concatenate(both, axis=1))
            for i, weights in enumerate(probs):
                both = jnp.dot(weights, values, preferred_element_type=f32)
                total = both[:, :half] / both[:, half:]
                at = pl.multiple_of((kv * pairs_per_kv + i) * half, half)
                heads[t, lo, :, pl.ds(at, half)] = total.astype(bf16)
            heads_copy(t, kv).start()
            if after is not None:
                after(kv)
            return carry

        lax.fori_loop(0, pairs // pairs_per_kv, group, 0)

    def out_dot(t, c):
        got = jnp.dot(heads[t, 0], w_out[0, c], preferred_element_type=f32)
        return got + jnp.dot(heads[t, 1], w_out[1, c], preferred_element_type=f32)

    def cross_copy(j, q):
        return remote(give.at[j, q], x_in.at[j, q], xs_s, xs_r.at[j, q], section, peer)

    def peer_output(t, j, c, send=True):
        got = out_dot(t, c).astype(bf16)
        for i in range(per_dot):
            give[j, c * per_dot + i] = got[:, i * cols : (i + 1) * cols]
            if send:
                cross_copy(j, c * per_dot + i).start()

    def own_output(t, j, c):
        got = out_dot(t, c)
        for i in range(per_dot):
            own_part[j, c * per_dot + i] = got[:, i * cols : (i + 1) * cols]

    def own_half(t, j, c, core):
        got = jnp.dot(heads[t, core], w_out[core, c], preferred_element_type=f32)
        for i in range(per_dot):
            part = got[:, i * cols : (i + 1) * cols]
            if core is lo:
                own_part[j, c * per_dot + i] = part
            else:
                own_part[j, c * per_dot + i] += part

    def loop(count, body):
        def step(i, carry):
            body(i)
            return carry

        lax.fori_loop(0, count, step, 0)

    def out_copy(j, q):
        return remote(
            mixed.at[j, q],
            out.at[0, :, pl.ds(pl.multiple_of(my_side + q * cols, cols), cols)],
            out_s,
            out_r.at[lo, q // PAIR],
            nxt,
            hi * 2 + j,
        )

    def hist_arrival(k, i, q):
        place = hist_in.at[k - 1, i, q]
        return remote(
            place, place, hist_s.at[k - 1], hist_r.at[k - 1, i, q], section, sibling
        )

    def history_of(k, i, q):
        @pl.when(q % per_past == 0)
        def _():
            hist_arrival(k, i, q // per_past).wait_recv()

        where = pl.ds(pl.multiple_of((q % per_past) * cols, cols), cols)
        return hist_in[k - 1, i, q // per_past, :, where].astype(f32)

    load_mix.wait()
    position = lax.broadcasted_iota(jnp.int32, mix_v.shape, 1)

    def factors_of(s):
        return jnp.sum(jnp.where(position == s, mix_v[...], 0.0), axis=1, keepdims=True)

    factors = factors_of(section)
    plain = jnp.where(section == last, jnp.ones_like(factors[0:1]), factors[0:1])

    def finish(j, q):
        cross_copy(j, q).wait_recv()
        total = own_part[j, q] + x_in[j, q].astype(f32)
        given = x_res[j, :, pl.ds(pl.multiple_of(q * cols, cols), cols)].astype(f32)
        block = (given + total).astype(bf16)
        acc[...] = plain * block.astype(f32)
        for k in range(1, slots + 1):

            @pl.when(gets[k - 1])
            def _():
                acc[...] += factors[k : k + 1] * history_of(k, j, q)

        mixed[j, q] = acc[...].astype(bf16)
        out_copy(j, q).start()

    def receive_block(j, then=None):
        def pass_on(i):
            gather_copy(j, i).wait_recv()
            forward_copy(j, i).start()

        def passed(count):
            settle(peer_rows.at[j, pl.ds(0, count * unit)], fw_r.at[j]).wait_recv()

        if j == 0:
            for i in range(share):
                pass_on(i)
            passed(share)
            return
        for i in range(share - 1):
            pass_on(i)

        @pl.when((hi == 1) & (lo == 1))
        def _():
            pass_on(share)

        @pl.when((hi == 0) | (lo == 1))
        def _():
            pass_on(share - 1)

        then()

        @pl.when(hi == 0)
        def _():
            passed(share)

        @pl.when((hi == 1) & (lo == 0))
        def _():
            passed(share + 1)

        @pl.when((hi == 1) & (lo == 1))
        def _():
            passed(share - 1)

    fill_ones()
    pltpu.make_async_copy(w_all, w_all, w_sem).wait()
    project_key_value(chip_rows, hi * 2)
    project_query(chip_rows, hi * 2 * rows)

    def out_weights_ready():
        pltpu.make_async_copy(w_out.at[lo], w_out.at[lo], wo_sem).wait()
        settle(w_out.at[1 - lo], wr_r).wait_recv()
        load_res.wait()
        residual_copy().wait_recv()

    def peer_block(j):
        target = ((1 - hi) * 2 + j) * rows
        return peer_rows.at[j], target

    @pl.when(hi == 0)
    def _():
        attend(0)
        attend(1)

    out_weights_ready()

    @pl.when(hi == 0)
    def _():
        for j in range(2):
            heads_ready(j)
            loop(DOTS, lambda c: own_output(j, j, c))

    for r in range(RELAYS):

        @pl.when(does_relay[r])
        def _():
            relay_in(r).wait_recv()
            relay_out(r).start()

    receive_block(0)
    project_key_value(peer_rows.at[0], (1 - hi) * 2)
    project_query(*peer_block(0))

    @pl.when(hi == 0)
    def _():
        attend(2)

        @pl.when(jnp.logical_not(host))
        def _():
            settle(peer_rows.at[0], gx_s).wait_send()
            settle(peer_rows.at[0, pl.ds(0, unit)], gx_s).wait_send()
            tell(clear_sem, sibling)
            heads_ready(2)
            loop(DOTS, lambda c: peer_output(2, 0, c))

        @pl.when(host)
        def _():
            heads_ready(2)
            loop(DOTS, lambda c: peer_output(2, 0, c, False))
            settle(peer_rows.at[0, pl.ds(0, rows - unit)], gx_s).wait_send()
            pl.semaphore_wait(clear_sem, 1)
            loop(CHUNKS, lambda q: cross_copy(0, q).start())


    @pl.when(hi == 1)
    def _():
        attend(0)
        heads_ready(0)
        loop(DOTS, lambda c: peer_output(0, 0, c))

    @pl.when(late & jnp.logical_not(latest))
    def _():
        send_history()

    def finish_part(j, c, parts=2):
        count = CHUNKS // (parts * DOTS)
        loop(count, lambda i: finish(j, c * count + i))

    def first_part():
        @pl.when(hi == 0)
        def _():
            finish_part(0, 0)

    receive_block(1, first_part)
    project_key_value(peer_rows.at[1], (1 - hi) * 2 + 1)

    @pl.when(hi == 0)
    def _():
        project_query(*peer_block(1))
        finish_part(0, 1)
        attend(3, lambda kv: finish_part(0, 2 + kv))

        @pl.when(latest)
        def _():
            send_history()

        finish_part(0, 4)
        heads_ready(3)

        def step(c):
            peer_output(3, 1, c)

            @pl.when(c > 0)
            def _():
                finish_part(0, 4 + c)

        loop(DOTS, step)
        loop(CHUNKS, lambda q: finish(1, q))

    @pl.when(hi == 1)
    def _():
        attend(2)
        own_half(2, 0, 0, lo)

        @pl.when(lo == 1)
        def _():
            project_query(*peer_block(1))

        heads_ready(2)
        own_half(2, 0, 0, 1 - lo)
        finish_part(0, 0, 1)

        @pl.when(lo == 0)
        def _():
            project_query(*peer_block(1))

        attend(1)

        @pl.when(latest)
        def _():
            send_history()

        own_output(2, 0, 1)
        finish_part(0, 1, 1)
        heads_ready(1)
        loop(DOTS, lambda c: peer_output(1, 1, c))
        own_output(2, 0, 2)
        finish_part(0, 2, 1)
        attend(3)
        own_output(2, 0, 3)
        finish_part(0, 3, 1)
        heads_ready(3)

        def second(c):
            own_output(3, 1, c)
            finish_part(1, c, 1)

        loop(DOTS, second)

    def out_arrival(c, q):
        span = PAIR * cols
        place = out.at[0, :, pl.ds(pl.multiple_of(c * side + q * span, span), span)]
        return settle(place, out_r.at[c, q])

    late_factors = factors_of(last)

    def take(q):
        for c in range(2):
            out_arrival(c, q).wait_recv()

            @pl.when(section == 0)
            def _():
                for i in range(PAIR):
                    at = q * PAIR + i
                    where = pl.ds(pl.multiple_of(c * side + at * cols, cols), cols)
                    acc[...] = late_factors[0:1] * out[0, :, where].astype(f32)
                    for k in range(1, slots + 1):

                        @pl.when(gets_last[k - 1])
                        def _():
                            acc[...] += late_factors[k : k + 1] * history_of(k, c, at)

                    out[0, :, where] = acc[...].astype(bf16)

    loop(CHUNKS // PAIR, take)

    settle(chip_rows.at[pl.ds(0, rows)], sib_s).wait_send()

    @pl.when(hi == 1)
    def _():
        settle(peer_rows.at[0], gx_s).wait_send()

    settle(peer_rows.at[0, pl.ds(0, rows - unit)], fw_s).wait_send()

    @pl.when((hi == 0) | (lo == 1))
    def _():
        settle(peer_rows.at[0, pl.ds(0, unit)], fw_s).wait_send()

    @pl.when((hi == 1) & (lo == 1))
    def _():
        settle(peer_rows.at[0, pl.ds(0, unit)], fw_s).wait_send()

    settle(w_out.at[lo], wr_s).wait_send()
    residual_copy().wait_send()
    settle(heads.at[:, lo], hd_s).wait_send()
    for k in range(1, slots + 1):

        @pl.when(gives[k - 1] | gives_last[k - 1])
        def _():
            settle(hist_in.at[k - 1], hist_s.at[k - 1]).wait_send()

    settle(give, xs_s).wait_send()
    settle(mixed, out_s).wait_send()

    for r in range(RELAYS):

        @pl.when(does_relay[r])
        def _():
            relay_out(r).wait_send()


def solution(mesh):
    sections, tensor = mesh.shape["section"], mesh.shape["tensor"]
    assert tensor == 4

    def on_device(x, history, wq, wk, wv, wo, mix_weights):
        rows, width = x.shape[1:]
        slots = history.shape[1]
        q_width, kv_width = wq.shape[2], wk.shape[2]
        seq = rows * tensor
        tile = 2 * kv_width
        q_tiles = q_width // tile
        side = width // 2
        wide, cols = side // DOTS, side // CHUNKS
        bf16, f32 = jnp.bfloat16, jnp.float32
        dma = pltpu.SemaphoreType.DMA
        hbm = pl.BlockSpec(memory_space=pltpu.HBM)
        factors = mix_weights.T
        return pl.pallas_call(
            functools.partial(tick_kernel, sections),
            out_shape=pltpu.VMEM(x.shape, bf16),
            in_specs=[hbm] * 7,
            out_specs=pl.BlockSpec(memory_space=pltpu.VMEM),
            scratch_shapes=[
                pltpu.VMEM((rows, width), bf16),
                pltpu.VMEM((2, rows, side), bf16),
                pltpu.VMEM((2 * rows, width), bf16),
                pltpu.VMEM((2, rows, width), bf16),
                pltpu.VMEM((q_tiles + 1, width, tile), bf16),
                pltpu.VMEM((2, DOTS, q_width, wide), bf16),
                pltpu.VMEM((2 * q_tiles, seq, kv_width), bf16),
                pltpu.VMEM((kv_width // HEAD_DIM, tensor, 2, rows, kv_width), bf16),
                pltpu.VMEM((kv_width // HEAD_DIM, tensor, 2, rows, 2 * kv_width), bf16),
                pltpu.VMEM((4, 2, rows, q_width), bf16),
                pltpu.VMEM((2, CHUNKS, rows, cols), f32),
                pltpu.VMEM((2, CHUNKS, rows, cols), bf16),
                pltpu.VMEM((2, CHUNKS, rows, cols), bf16),
                pltpu.VMEM((2, CHUNKS, rows, cols), bf16),
                pltpu.VMEM((rows, cols), f32),
                pltpu.VMEM((slots, 2, PASTS, rows, side // PASTS), bf16),
                pltpu.VMEM(factors.shape, factors.dtype),
                dma,
                dma,
                dma((3,)),
                dma,
                dma,
                dma((slots,)),
                dma((slots, 2, PASTS)),
                dma,
                dma,
                dma,
                dma((2, UNITS // 2 + 1)),
                dma,
                dma((2,)),
                dma,
                dma,
                dma,
                dma,
                dma,
                dma((4,)),
                dma,
                dma((2, CHUNKS)),
                dma,
                dma((2, CHUNKS // PAIR)),
                pltpu.VMEM((RELAYS, rows // UNITS, width), bf16),
                dma((RELAYS,)),
                dma((RELAYS,)),
                pltpu.SemaphoreType.REGULAR,
                pltpu.SemaphoreType.REGULAR,
                pltpu.SemaphoreType.REGULAR,
            ],
            compiler_params=pltpu.CompilerParams(
                collective_id=0, has_side_effects=True, vmem_limit_bytes=56 * 1024 * 1024
            ),
        )(x, history, wq, wk, wv, wo, factors)

    placed = (
        P("section", "tensor", None),
        P("section", None, "tensor", None),
        P("section", None, "tensor"),
        P("section", None, "tensor"),
        P("section", None, "tensor"),
        P("section", "tensor", None),
        P(),
    )
    return jax.shard_map(
        on_device,
        mesh=mesh,
        in_specs=placed,
        out_specs=P("section", "tensor", None),
        check_vma=False,
    )
```

```python
import functools
import math

import jax
import jax.numpy as jnp
from jax import lax
from jax.experimental import pallas as pl
from jax.experimental.pallas import tpu as pltpu
from jax.sharding import PartitionSpec as P

HEAD_DIM = 64
DILATION_STRIDE = 4
MESH = pl.DeviceIdType.MESH
UNITS = 8
DOTS = 4
CHUNKS = 16
PASTS = 4
PAIR = 4
RELAYS = 1


def start(copy):
    copy.start()
    return copy


def tick_kernel(
    sections,
    x_hbm,
    hist_hbm,
    wq_hbm,
    wk_hbm,
    wv_hbm,
    wo_hbm,
    mix_hbm,
    out,
    x_own,
    x_res,
    chip_rows,
    peer_rows,
    w_all,
    w_out,
    q_all,
    k_pad,
    v_pad,
    heads,
    own_part,
    give,
    x_in,
    mixed,
    acc,
    hist_in,
    mix_v,
    w_sem,
    wo_sem,
    x_sem,
    res_sem,
    mix_sem,
    hist_s,
    hist_r,
    sib_s,
    sib_r,
    gx_s,
    gx_r,
    fw_s,
    fw_r,
    wr_s,
    wr_r,
    xr_s,
    xr_r,
    hd_s,
    hd_r,
    xs_s,
    xs_r,
    out_s,
    out_r,
    relay,
    relay_s,
    relay_r,
    near_sem,
    far_sem,
    clear_sem,
):
    section = lax.axis_index("section")
    me = lax.axis_index("tensor")
    hi, lo = me // 2, me % 2
    sibling = hi * 2 + (1 - lo)
    peer = (1 - hi) * 2 + lo
    rows, width = x_own.shape
    slots = hist_in.shape[0]
    unit = rows // UNITS
    side = width // 2
    wide = side // DOTS
    cols = side // CHUNKS
    per_dot = CHUNKS // DOTS
    past = side // PASTS
    per_past = CHUNKS // PASTS
    q_tiles = w_all.shape[0] - 1
    tile = w_all.shape[2]
    half = tile // 2
    last = sections - 1
    nxt = lax.rem(section + 1, sections)
    prv = lax.rem(section + sections - 1, sections)
    f32, bf16 = jnp.float32, jnp.bfloat16

    middle = (section > 0) & (section < last)
    gets = [middle & (section >= DILATION_STRIDE * k) for k in range(1, slots + 1)]
    gets_last = [(section == 0) & (last >= DILATION_STRIDE * k) for k in range(1, slots + 1)]
    gives = [section + DILATION_STRIDE * k < last for k in range(1, slots + 1)]
    gives_last = [section + DILATION_STRIDE * k == last for k in range(1, slots + 1)]

    def load_unit(i):
        if i < 2:
            at = pl.ds(pl.multiple_of(order[i] * unit, unit), unit)
        else:
            at = pl.ds(2 * unit, rows - 2 * unit)
        return pltpu.make_async_copy(x_hbm.at[0, at], x_own.at[at], x_sem.at[i])

    order = [lo, 1 - lo] + list(range(2, UNITS))
    for i in range(3):
        load_unit(i).start()
    barrier = pltpu.get_barrier_semaphore()

    def greet(s, t):
        pl.semaphore_signal(
            barrier, inc=1, device_id={"section": s, "tensor": t}, device_id_type=MESH
        )

    host = hi == lo
    keeper = hi * 2 + (1 - hi)

    @pl.when(jnp.logical_not(host))
    def _():
        greet(section, sibling)
        greet(section, peer)

    greet(prv, keeper)
    expected = jnp.int32(2)
    for k in range(1, slots + 1):
        step = DILATION_STRIDE * k

        @pl.when(gets[k - 1])
        def _():
            greet(section - step, keeper)

        @pl.when(gets_last[k - 1])
        def _():
            greet(last - step, keeper)

        expected = expected + 2 * (gives[k - 1] | gives_last[k - 1]).astype(jnp.int32)

    vias = [max(last - 2 - r, 0) for r in range(RELAYS)]
    sends_relay = (section == last) & (lo == 1)
    does_relay = [(section == via) & (lo == 1) for via in vias]
    expected = expected + RELAYS * (section == last).astype(jnp.int32)
    for via, does in zip(vias, does_relay):

        @pl.when(does)
        def _():
            greet(last, (1 - hi) * 2 + hi)

        @pl.when(sends_relay)
        def _():
            greet(via, keeper)

        expected = expected + (section == via).astype(jnp.int32)

    loads = [
        pltpu.make_async_copy(
            wk_hbm.at[0], w_all.at[q_tiles, :, pl.ds(0, half)], w_sem
        ),
        pltpu.make_async_copy(
            wv_hbm.at[0], w_all.at[q_tiles, :, pl.ds(half, half)], w_sem
        ),
    ]
    for j in range(q_tiles):
        loads.append(
            pltpu.make_async_copy(
                wq_hbm.at[0, :, pl.ds(j * tile, tile)], w_all.at[j], w_sem
            )
        )
    for copy in loads:
        copy.start()
    load_mix = start(pltpu.make_async_copy(mix_hbm, mix_v, mix_sem))
    mine = pl.multiple_of(lo * rows, rows)
    my_side = pl.multiple_of(lo * side, side)
    other_side = pl.multiple_of((1 - lo) * side, side)

    def norm_unit(u):
        def norm_rows(i, carry):
            at = pl.multiple_of(u * unit + i * 16, 16)
            values = x_own[pl.ds(at, 16), :].astype(f32)
            inv = lax.rsqrt(jnp.mean(values * values, axis=-1, keepdims=True) + 1e-05)
            chip_rows[pl.ds(pl.multiple_of(mine + at, 16), 16), :] = (values * inv).astype(bf16)
            return carry

        lax.fori_loop(0, unit // 16, norm_rows, 0)

    def remote(src, dst, send, recv, s, t):
        return pltpu.make_async_remote_copy(
            src_ref=src,
            dst_ref=dst,
            send_sem=send,
            recv_sem=recv,
            device_id={"section": s, "tensor": t},
            device_id_type=MESH,
        )

    def settle(place, sem):
        return remote(place, place, sem, sem, section, sibling)

    def sibling_copy(u):
        place = chip_rows.at[pl.ds(pl.multiple_of(mine + u * unit, unit), unit)]
        return remote(place, place, sib_s, sib_r, section, sibling)

    share = UNITS // 2

    def unit_of(i):
        return UNITS - 2 if i == share else 2 * i + lo

    def gather_copy(j, i):
        at = unit_of(i) * unit
        return remote(
            chip_rows.at[pl.ds(pl.multiple_of(j * rows + at, unit), unit)],
            peer_rows.at[j, pl.ds(pl.multiple_of(at, unit), unit)],
            gx_s,
            gx_r.at[j, i],
            section,
            peer,
        )

    def forward_copy(j, i):
        place = peer_rows.at[j, pl.ds(pl.multiple_of(unit_of(i) * unit, unit), unit)]
        return remote(place, place, fw_s, fw_r.at[j], section, sibling)

    def hist_copy(k, c, q, to_last):
        src = hist_hbm.at[0, k - 1, :, pl.ds(pl.multiple_of(c * side + q * past, past), past)]
        slot = c if to_last else lo
        if to_last:
            s, t = 0, me
        else:
            s, t = section + DILATION_STRIDE * k, hi * 2 + c
        return remote(
            src,
            hist_in.at[k - 1, slot, q],
            hist_s.at[k - 1],
            hist_r.at[k - 1, slot, q],
            s,
            t,
        )

    def send_history():
        for k in range(1, slots + 1):
            for to_last, sends in ((False, gives[k - 1]), (True, gives_last[k - 1])):

                @pl.when(sends)
                def _():
                    def each(q, carry):
                        for c in range(2):
                            hist_copy(k, c, q, to_last).start()
                        return carry

                    lax.fori_loop(0, PASTS, each, 0)

    late = (lo == 1) & (section % 2 == 0)
    latest = late & (section % DILATION_STRIDE == 0)

    def tell(sem, t):
        pl.semaphore_signal(
            sem, inc=1, device_id={"section": section, "tensor": t}, device_id_type=MESH
        )

    load_unit(0).wait()
    norm_unit(order[0])

    @pl.when(host)
    def _():
        pl.semaphore_wait(barrier, 2)
        gather_copy(lo, 0).start()
        tell(near_sem, sibling)
        tell(near_sem, peer)
        sibling_copy(order[0]).start()

    load_unit(1).wait()
    norm_unit(order[1])

    @pl.when(jnp.logical_not(host))
    def _():
        pl.semaphore_wait(near_sem, 2)
        gather_copy(lo, 0).start()
        sibling_copy(order[0]).start()

    sibling_copy(order[1]).start()
    load_unit(2).wait()
    for i in range(2, UNITS):
        norm_unit(order[i])
        sibling_copy(order[i]).start()
        if i % 2 == 0:

            @pl.when(lo == 0)
            def _():
                gather_copy(0, i // 2).start()

    settle(chip_rows.at[pl.ds(0, rows)], sib_r).wait_recv()

    @pl.when(lo == 0)
    def _():
        for i in range(share - 1):
            gather_copy(1, i).start()

        @pl.when(hi == 1)
        def _():
            gather_copy(1, share - 1).start()

    @pl.when(lo == 1)
    def _():
        for i in range(share):
            gather_copy(0, i).start()
        for i in range(1, share - RELAYS):
            gather_copy(1, i).start()

        @pl.when(hi == 0)
        def _():
            gather_copy(1, share).start()

        @pl.when(section < last)
        def _():
            for i in range(share - RELAYS, share):
                gather_copy(1, i).start()

    @pl.when(jnp.logical_not(host))
    def _():
        pl.semaphore_wait(barrier, expected)
        tell(far_sem, sibling)

    @pl.when(host)
    def _():
        pl.semaphore_wait(far_sem, 1)

    def relay_in(r):
        src = chip_rows.at[pl.ds(2 * rows - (2 * r + 1) * unit, unit)]
        return remote(src, relay.at[r], gx_s, relay_r.at[r], vias[r], peer)

    def relay_out(r):
        place = peer_rows.at[1, pl.ds(rows - (2 * r + 1) * unit, unit)]
        return remote(
            relay.at[r], place, relay_s.at[r], gx_r.at[1, share - 1 - r], last, me
        )

    @pl.when(sends_relay)
    def _():
        for r in range(RELAYS):
            relay_in(r).start()

    @pl.when(jnp.logical_not(late))
    def _():
        send_history()

    def weight_copy(c):
        return remote(
            wo_hbm.at[0, :, pl.ds(pl.multiple_of(other_side + c * wide, wide), wide)],
            w_out.at[lo, c],
            wr_s,
            wr_r,
            section,
            sibling,
        )

    def residual_copy():
        return remote(
            x_own.at[:, pl.ds(other_side, side)], x_res.at[lo], xr_s, xr_r, section, sibling
        )

    for c in range(DOTS):
        pltpu.make_async_copy(
            wo_hbm.at[0, :, pl.ds(pl.multiple_of(my_side + c * wide, wide), wide)],
            w_out.at[lo, c],
            wo_sem,
        ).start()
        weight_copy(c).start()
    load_res = start(
        pltpu.make_async_copy(x_hbm.at[0, :, pl.ds(my_side, side)], x_res.at[lo], res_sem)
    )
    residual_copy().start()

    scale = 1.0 / math.sqrt(HEAD_DIM)

    def project_query(rows_ref, target):
        size = rows_ref.shape[0]
        where = pl.ds(pl.multiple_of(target, size), size)

        def q_tile(j, carry):
            got = jnp.dot(rows_ref[...], w_all[j], preferred_element_type=f32)
            got = got.astype(bf16) * bf16(scale)
            q_all[2 * j, where, :] = got[:, :half]
            q_all[2 * j + 1, where, :] = got[:, half:]
            return carry

        lax.fori_loop(0, q_tiles, q_tile, 0)

    def project_key_value(rows_ref, first):
        size = rows_ref.shape[0]
        got = jnp.dot(rows_ref[...], w_all[q_tiles], preferred_element_type=f32)
        got = got.astype(bf16).astype(f32)
        for part, padded in ((got[:, :half], k_pad), (got[:, half:], v_pad)):
            lane = lax.broadcasted_iota(jnp.int32, part.shape, 1)
            turned = pltpu.roll(part, HEAD_DIM, 1)
            low = lane < HEAD_DIM
            zero = jnp.zeros_like(part)
            forms = (
                jnp.where(low, part, zero),
                jnp.where(low, zero, turned),
                jnp.where(low, turned, zero),
                jnp.where(low, zero, part),
            )
            for f, form in enumerate(forms):
                for i in range(size // rows):
                    some = form[i * rows : (i + 1) * rows].astype(bf16)
                    padded[f // 2, first + i, f % 2, :, :half] = some

    def fill_ones():
        low = lax.broadcasted_iota(jnp.int32, (rows, half), 1) < HEAD_DIM
        for which in range(2):
            ones = jnp.where(low == (which == 0), 1.0, 0.0).astype(bf16)
            for kv in range(v_pad.shape[0]):
                for i in range(v_pad.shape[1]):
                    v_pad[kv, i, which, :, half:] = ones

    pairs = q_all.shape[0]
    pairs_per_kv = pairs // (half // HEAD_DIM)

    def heads_copy(t, kv):
        span = pairs_per_kv * half
        place = heads.at[t, lo, :, pl.ds(pl.multiple_of(kv * span, span), span)]
        return remote(place, place, hd_s, hd_r.at[t], section, sibling)

    def heads_ready(t):
        settle(heads.at[t, 1 - lo], hd_r.at[t]).wait_recv()

    def attend(t, after=None):
        first, blocks = t * rows, t + 1
        seen = lax.broadcasted_iota(jnp.int32, (rows, rows), 0) >= lax.broadcasted_iota(
            jnp.int32, (rows, rows), 1
        )

        def exponents(scores, which):
            mine = [
                scores[:, (2 * i + which) * rows : (2 * i + which + 1) * rows]
                for i in range(blocks)
            ]
            mine[t] = jnp.where(seen, mine[t], -1e30)
            top = jnp.max(functools.reduce(jnp.maximum, mine), axis=-1, keepdims=True)
            return [jnp.exp(part - top).astype(bf16) for part in mine]

        def group(kv, carry):
            keys = k_pad[kv, :blocks].reshape(2 * blocks * rows, half)
            values = v_pad[kv, :blocks].reshape(2 * blocks * rows, 2 * half)
            scores = [
                lax.dot_general(
                    q_all[kv * pairs_per_kv + i, first : first + rows, :],
                    keys,
                    (((1,), (1,)), ((), ())),
                    preferred_element_type=f32,
                )
                for i in range(pairs_per_kv)
            ]
            probs = []
            for got in scores:
                even, odd = exponents(got, 0), exponents(got, 1)
                both = [part for pair in zip(even, odd) for part in pair]
                probs.append(jnp.concatenate(both, axis=1))
            for i, weights in enumerate(probs):
                both = jnp.dot(weights, values, preferred_element_type=f32)
                total = both[:, :half] / both[:, half:]
                at = pl.multiple_of((kv * pairs_per_kv + i) * half, half)
                heads[t, lo, :, pl.ds(at, half)] = total.astype(bf16)
            heads_copy(t, kv).start()
            if after is not None:
                after(kv)
            return carry

        lax.fori_loop(0, pairs // pairs_per_kv, group, 0)

    def out_dot(t, c):
        got = jnp.dot(heads[t, 0], w_out[0, c], preferred_element_type=f32)
        return got + jnp.dot(heads[t, 1], w_out[1, c], preferred_element_type=f32)

    def cross_copy(j, q):
        return remote(give.at[j, q], x_in.at[j, q], xs_s, xs_r.at[j, q], section, peer)

    def peer_output(t, j, c, send=True):
        got = out_dot(t, c).astype(bf16)
        for i in range(per_dot):
            give[j, c * per_dot + i] = got[:, i * cols : (i + 1) * cols]
            if send:
                cross_copy(j, c * per_dot + i).start()

    def own_output(t, j, c):
        got = out_dot(t, c)
        for i in range(per_dot):
            own_part[j, c * per_dot + i] = got[:, i * cols : (i + 1) * cols]

    def own_half(t, j, c, core):
        got = jnp.dot(heads[t, core], w_out[core, c], preferred_element_type=f32)
        for i in range(per_dot):
            part = got[:, i * cols : (i + 1) * cols]
            if core is lo:
                own_part[j, c * per_dot + i] = part
            else:
                own_part[j, c * per_dot + i] += part

    def loop(count, body):
        def step(i, carry):
            body(i)
            return carry

        lax.fori_loop(0, count, step, 0)

    def out_copy(j, q):
        return remote(
            mixed.at[j, q],
            out.at[0, :, pl.ds(pl.multiple_of(my_side + q * cols, cols), cols)],
            out_s,
            out_r.at[lo, q // PAIR],
            nxt,
            hi * 2 + j,
        )

    def hist_arrival(k, i, q):
        place = hist_in.at[k - 1, i, q]
        return remote(
            place, place, hist_s.at[k - 1], hist_r.at[k - 1, i, q], section, sibling
        )

    def history_of(k, i, q):
        @pl.when(q % per_past == 0)
        def _():
            hist_arrival(k, i, q // per_past).wait_recv()

        where = pl.ds(pl.multiple_of((q % per_past) * cols, cols), cols)
        return hist_in[k - 1, i, q // per_past, :, where].astype(f32)

    load_mix.wait()
    position = lax.broadcasted_iota(jnp.int32, mix_v.shape, 1)

    def factors_of(s):
        return jnp.sum(jnp.where(position == s, mix_v[...], 0.0), axis=1, keepdims=True)

    factors = factors_of(section)
    plain = jnp.where(section == last, jnp.ones_like(factors[0:1]), factors[0:1])

    def finish(j, q):
        cross_copy(j, q).wait_recv()
        total = own_part[j, q] + x_in[j, q].astype(f32)
        given = x_res[j, :, pl.ds(pl.multiple_of(q * cols, cols), cols)].astype(f32)
        block = (given + total).astype(bf16)
        acc[...] = plain * block.astype(f32)
        for k in range(1, slots + 1):

            @pl.when(gets[k - 1])
            def _():
                acc[...] += factors[k : k + 1] * history_of(k, j, q)

        mixed[j, q] = acc[...].astype(bf16)
        out_copy(j, q).start()

    def receive_block(j, then=None):
        def pass_on(i):
            gather_copy(j, i).wait_recv()
            forward_copy(j, i).start()

        def passed(count):
            settle(peer_rows.at[j, pl.ds(0, count * unit)], fw_r.at[j]).wait_recv()

        if j == 0:
            for i in range(share):
                pass_on(i)
            passed(share)
            return
        for i in range(share - 1):
            pass_on(i)

        @pl.when((hi == 1) & (lo == 1))
        def _():
            pass_on(share)

        @pl.when((hi == 0) | (lo == 1))
        def _():
            pass_on(share - 1)

        then()

        @pl.when(hi == 0)
        def _():
            passed(share)

        @pl.when((hi == 1) & (lo == 0))
        def _():
            passed(share + 1)

        @pl.when((hi == 1) & (lo == 1))
        def _():
            passed(share - 1)

    fill_ones()
    pltpu.make_async_copy(w_all, w_all, w_sem).wait()
    project_key_value(chip_rows, hi * 2)
    project_query(chip_rows, hi * 2 * rows)

    def out_weights_ready():
        pltpu.make_async_copy(w_out.at[lo], w_out.at[lo], wo_sem).wait()
        settle(w_out.at[1 - lo], wr_r).wait_recv()
        load_res.wait()
        residual_copy().wait_recv()

    def peer_block(j):
        target = ((1 - hi) * 2 + j) * rows
        return peer_rows.at[j], target

    @pl.when(hi == 0)
    def _():
        attend(0)
        attend(1)

    out_weights_ready()

    @pl.when(hi == 0)
    def _():
        for j in range(2):
            heads_ready(j)
            loop(DOTS, lambda c: own_output(j, j, c))

    for r in range(RELAYS):

        @pl.when(does_relay[r])
        def _():
            relay_in(r).wait_recv()
            relay_out(r).start()

    receive_block(0)
    project_key_value(peer_rows.at[0], (1 - hi) * 2)
    project_query(*peer_block(0))

    @pl.when(hi == 0)
    def _():
        attend(2)

        @pl.when(jnp.logical_not(host))
        def _():
            settle(peer_rows.at[0], gx_s).wait_send()
            settle(peer_rows.at[0, pl.ds(0, unit)], gx_s).wait_send()
            tell(clear_sem, sibling)
            heads_ready(2)
            loop(DOTS, lambda c: peer_output(2, 0, c))

        @pl.when(host)
        def _():
            heads_ready(2)
            loop(DOTS, lambda c: peer_output(2, 0, c, False))
            settle(peer_rows.at[0, pl.ds(0, rows - unit)], gx_s).wait_send()
            pl.semaphore_wait(clear_sem, 1)
            loop(CHUNKS, lambda q: cross_copy(0, q).start())


    @pl.when(hi == 1)
    def _():
        attend(0)
        heads_ready(0)
        loop(DOTS, lambda c: peer_output(0, 0, c))

    @pl.when(late & jnp.logical_not(latest))
    def _():
        send_history()

    def finish_part(j, c, parts=2):
        count = CHUNKS // (parts * DOTS)
        loop(count, lambda i: finish(j, c * count + i))

    def first_part():
        @pl.when(hi == 0)
        def _():
            finish_part(0, 0)

    receive_block(1, first_part)
    project_key_value(peer_rows.at[1], (1 - hi) * 2 + 1)

    @pl.when(hi == 0)
    def _():
        project_query(*peer_block(1))
        finish_part(0, 1)
        attend(3, lambda kv: finish_part(0, 2 + kv))

        @pl.when(latest)
        def _():
            send_history()

        finish_part(0, 4)
        heads_ready(3)

        def step(c):
            peer_output(3, 1, c)

            @pl.when(c > 0)
            def _():
                finish_part(0, 4 + c)

        loop(DOTS, step)
        loop(CHUNKS, lambda q: finish(1, q))

    @pl.when(hi == 1)
    def _():
        attend(2)
        own_half(2, 0, 0, lo)

        @pl.when(lo == 1)
        def _():
            project_query(*peer_block(1))

        heads_ready(2)
        own_half(2, 0, 0, 1 - lo)
        finish_part(0, 0, 1)

        @pl.when(lo == 0)
        def _():
            project_query(*peer_block(1))

        attend(1)

        @pl.when(latest)
        def _():
            send_history()

        own_output(2, 0, 1)
        finish_part(0, 1, 1)
        heads_ready(1)
        loop(DOTS, lambda c: peer_output(1, 1, c))
        own_output(2, 0, 2)
        finish_part(0, 2, 1)
        attend(3)
        own_output(2, 0, 3)
        finish_part(0, 3, 1)
        heads_ready(3)

        def second(c):
            own_output(3, 1, c)
            finish_part(1, c, 1)

        loop(DOTS, second)

    def out_arrival(c, q):
        span = PAIR * cols
        place = out.at[0, :, pl.ds(pl.multiple_of(c * side + q * span, span), span)]
        return settle(place, out_r.at[c, q])

    late_factors = factors_of(last)

    def take(q):
        for c in range(2):
            out_arrival(c, q).wait_recv()

            @pl.when(section == 0)
            def _():
                for i in range(PAIR):
                    at = q * PAIR + i
                    where = pl.ds(pl.multiple_of(c * side + at * cols, cols), cols)
                    acc[...] = late_factors[0:1] * out[0, :, where].astype(f32)
                    for k in range(1, slots + 1):

                        @pl.when(gets_last[k - 1])
                        def _():
                            acc[...] += late_factors[k : k + 1] * history_of(k, c, at)

                    out[0, :, where] = acc[...].astype(bf16)

    loop(CHUNKS // PAIR, take)

    settle(chip_rows.at[pl.ds(0, rows)], sib_s).wait_send()

    @pl.when(hi == 1)
    def _():
        settle(peer_rows.at[0], gx_s).wait_send()

    settle(peer_rows.at[0, pl.ds(0, rows - unit)], fw_s).wait_send()

    @pl.when((hi == 0) | (lo == 1))
    def _():
        settle(peer_rows.at[0, pl.ds(0, unit)], fw_s).wait_send()

    @pl.when((hi == 1) & (lo == 1))
    def _():
        settle(peer_rows.at[0, pl.ds(0, unit)], fw_s).wait_send()

    settle(w_out.at[lo], wr_s).wait_send()
    residual_copy().wait_send()
    settle(heads.at[:, lo], hd_s).wait_send()
    for k in range(1, slots + 1):

        @pl.when(gives[k - 1] | gives_last[k - 1])
        def _():
            settle(hist_in.at[k - 1], hist_s.at[k - 1]).wait_send()

    settle(give, xs_s).wait_send()
    settle(mixed, out_s).wait_send()

    for r in range(RELAYS):

        @pl.when(does_relay[r])
        def _():
            relay_out(r).wait_send()


def solution(mesh):
    sections, tensor = mesh.shape["section"], mesh.shape["tensor"]
    assert tensor == 4

    def on_device(x, history, wq, wk, wv, wo, mix_weights):
        rows, width = x.shape[1:]
        slots = history.shape[1]
        q_width, kv_width = wq.shape[2], wk.shape[2]
        seq = rows * tensor
        tile = 2 * kv_width
        q_tiles = q_width // tile
        side = width // 2
        wide, cols = side // DOTS, side // CHUNKS
        bf16, f32 = jnp.bfloat16, jnp.float32
        dma = pltpu.SemaphoreType.DMA
        hbm = pl.BlockSpec(memory_space=pltpu.HBM)
        factors = mix_weights.T
        return pl.pallas_call(
            functools.partial(tick_kernel, sections),
            out_shape=pltpu.VMEM(x.shape, bf16),
            in_specs=[hbm] * 7,
            out_specs=pl.BlockSpec(memory_space=pltpu.VMEM),
            scratch_shapes=[
                pltpu.VMEM((rows, width), bf16),
                pltpu.VMEM((2, rows, side), bf16),
                pltpu.VMEM((2 * rows, width), bf16),
                pltpu.VMEM((2, rows, width), bf16),
                pltpu.VMEM((q_tiles + 1, width, tile), bf16),
                pltpu.VMEM((2, DOTS, q_width, wide), bf16),
                pltpu.VMEM((2 * q_tiles, seq, kv_width), bf16),
                pltpu.VMEM((kv_width // HEAD_DIM, tensor, 2, rows, kv_width), bf16),
                pltpu.VMEM((kv_width // HEAD_DIM, tensor, 2, rows, 2 * kv_width), bf16),
                pltpu.VMEM((4, 2, rows, q_width), bf16),
                pltpu.VMEM((2, CHUNKS, rows, cols), f32),
                pltpu.VMEM((2, CHUNKS, rows, cols), bf16),
                pltpu.VMEM((2, CHUNKS, rows, cols), bf16),
                pltpu.VMEM((2, CHUNKS, rows, cols), bf16),
                pltpu.VMEM((rows, cols), f32),
                pltpu.VMEM((slots, 2, PASTS, rows, side // PASTS), bf16),
                pltpu.VMEM(factors.shape, factors.dtype),
                dma,
                dma,
                dma((3,)),
                dma,
                dma,
                dma((slots,)),
                dma((slots, 2, PASTS)),
                dma,
                dma,
                dma,
                dma((2, UNITS // 2 + 1)),
                dma,
                dma((2,)),
                dma,
                dma,
                dma,
                dma,
                dma,
                dma((4,)),
                dma,
                dma((2, CHUNKS)),
                dma,
                dma((2, CHUNKS // PAIR)),
                pltpu.VMEM((RELAYS, rows // UNITS, width), bf16),
                dma((RELAYS,)),
                dma((RELAYS,)),
                pltpu.SemaphoreType.REGULAR,
                pltpu.SemaphoreType.REGULAR,
                pltpu.SemaphoreType.REGULAR,
            ],
            compiler_params=pltpu.CompilerParams(
                collective_id=0, has_side_effects=True, vmem_limit_bytes=56 * 1024 * 1024
            ),
        )(x, history, wq, wk, wv, wo, factors)

    placed = (
        P("section", "tensor", None),
        P("section", None, "tensor", None),
        P("section", None, "tensor"),
        P("section", None, "tensor"),
        P("section", None, "tensor"),
        P("section", "tensor", None),
        P(),
    )
    return jax.shard_map(
        on_device,
        mesh=mesh,
        in_specs=placed,
        out_specs=P("section", "tensor", None),
        check_vma=False,
    )
```
